16 devices in a mesh: dp: 2 (over z), sp: 8 (over y, x, core).
Axes of the slice: x: 2, y: 2, z: 2, core: 2. Of those that a mesh axis runs over, the one named last changes fastest.
Arguments:
- hidden: bfloat16 [12288, 2048], P(('dp', 'sp')), parts along dimension 0
- positions: int32 [12288], P(('dp', 'sp')), parts along dimension 0
- d_attn: bfloat16 [12288, 2048], P(('dp', 'sp')), parts along dimension 0
- ln_weight: bfloat16 [2048], replicated
- w_q: bfloat16 [2048, 2048], replicated
- w_k: bfloat16 [2048, 2048], replicated
- w_v: bfloat16 [2048, 2048], replicated
- w_o: bfloat16 [2048, 2048], replicated
Outputs:
- output 1: bfloat16 [12288, 2048], P(('dp', 'sp')), parts along dimension 0
- output 2: bfloat16 [12288, 2048], P(('dp', 'sp')), parts along dimension 0
- output 3: bfloat16 [4096], P('dp'), parts along dimension 0
- output 4: bfloat16 [4096, 2048], P('dp'), parts along dimension 0
- output 5: bfloat16 [4096, 2048], P('dp'), parts along dimension 0
- output 6: bfloat16 [4096, 2048], P('dp'), parts along dimension 0
- output 7: bfloat16 [4096, 2048], P('dp'), parts along dimension 0
There are 2 independent parts. The reference program is written for one: setup_inputs(seed, part) draws one part's arguments, and reference() takes and returns one part's arrays. A program takes and returns all parts, laid end to end along the dimension named above; an argument that names none is the same for every part.
All inputs are finite; a program needn't handle non-finite values.
Results may differ from the reference program's by a relative error of at most 0.0122763.
Values are sent between devices in bfloat16 or wider.
A program may use at most 1 GiB of HBM per device.

```python
import math
import jax
import jax.numpy as jnp
from jax import lax

MODEL_DIM = 2048
NUM_HEADS = 16
NUM_KV_HEADS = 16
HEAD_DIM = 128
SEQ_LEN = 6144
LN_EPS = 1e-5
ROPE_BASE = 10000.0
GROUP_SIZE = NUM_HEADS // NUM_KV_HEADS
ROW_BLOCK = math.gcd(SEQ_LEN, 64)
NUM_BLOCKS = SEQ_LEN // ROW_BLOCK
SCORE_SCALE = HEAD_DIM ** -0.5


def setup_inputs(seed: int = 0, part: int = 0) -> dict:
    base_key = jax.random.key(seed)
    part_keys = jax.random.split(jax.random.fold_in(base_key, part), 3)
    weight_keys = jax.random.split(base_key, 5)
    hidden = jax.random.normal(part_keys[0], (SEQ_LEN, MODEL_DIM), jnp.float32).astype(jnp.bfloat16)
    pos_steps = jax.random.randint(part_keys[1], (SEQ_LEN,), 1, 4, dtype=jnp.int32)
    positions = (jnp.cumsum(pos_steps) - pos_steps[0]).astype(jnp.int32)
    d_attn = jax.random.normal(part_keys[2], (SEQ_LEN, MODEL_DIM), jnp.float32).astype(jnp.bfloat16)
    ln_weight = (1.0 + 0.25 * jax.random.normal(weight_keys[0], (MODEL_DIM,), jnp.float32)).astype(jnp.bfloat16)
    q_scale = math.sqrt(math.log(SEQ_LEN) / MODEL_DIM)
    kv_scale = MODEL_DIM ** -0.5
    o_scale = (NUM_HEADS * HEAD_DIM) ** -0.5
    w_q = (jax.random.normal(weight_keys[1], (MODEL_DIM, NUM_HEADS * HEAD_DIM), jnp.float32) * q_scale).astype(jnp.bfloat16)
    w_k = (jax.random.normal(weight_keys[2], (MODEL_DIM, NUM_KV_HEADS * HEAD_DIM), jnp.float32) * kv_scale).astype(jnp.bfloat16)
    w_v = (jax.random.normal(weight_keys[3], (MODEL_DIM, NUM_KV_HEADS * HEAD_DIM), jnp.float32) * kv_scale).astype(jnp.bfloat16)
    w_o = (jax.random.normal(weight_keys[4], (NUM_HEADS * HEAD_DIM, MODEL_DIM), jnp.float32) * o_scale).astype(jnp.bfloat16)
    return {'hidden': hidden, 'positions': positions, 'd_attn': d_attn, 'ln_weight': ln_weight,
            'w_q': w_q, 'w_k': w_k, 'w_v': w_v, 'w_o': w_o}


def norm_f32(hid_f32, weight_f32):
    mean_val = jnp.mean(hid_f32, axis=-1, keepdims=True)
    centered = hid_f32 - mean_val
    var_val = jnp.mean(centered * centered, axis=-1, keepdims=True)
    return centered * lax.rsqrt(var_val + LN_EPS) * weight_f32


def rope_tables(positions):
    inv_freq = ROPE_BASE ** (-jnp.arange(0, HEAD_DIM, 2, dtype=jnp.float32) / HEAD_DIM)
    angles = positions.astype(jnp.float32)[:, None] * inv_freq[None, :]
    return jnp.cos(angles)[:, None, :], jnp.sin(angles)[:, None, :]


def apply_rope(values, cos_t, sin_t):
    rot_pairs = values.reshape(values.shape[:-1] + (HEAD_DIM // 2, 2))
    even_part = rot_pairs[..., 0]
    odd_part = rot_pairs[..., 1]
    new_even = even_part * cos_t - odd_part * sin_t
    new_odd = odd_part * cos_t + even_part * sin_t
    return jnp.stack([new_even, new_odd], axis=-1).reshape(values.shape)


def block_probs(q_f32, row_start, k_f32):
    scores = jnp.einsum('qgrd,kgd->grqk', q_f32, k_f32) * SCORE_SCALE
    row_ids = row_start + jnp.arange(ROW_BLOCK)
    col_ids = jnp.arange(SEQ_LEN)
    scores = jnp.where(row_ids[:, None] >= col_ids[None, :], scores, -jnp.inf)
    return jax.nn.softmax(scores, axis=-1)


def reference(hidden, positions, d_attn, ln_weight, w_q, w_k, w_v, w_o):
    normed32, norm_vjp = jax.vjp(norm_f32, hidden.astype(jnp.float32), ln_weight.astype(jnp.float32))
    normed = normed32.astype(jnp.bfloat16)
    cos_t, sin_t = rope_tables(positions)
    q_rot = apply_rope(jnp.dot(normed, w_q, preferred_element_type=jnp.float32).reshape(SEQ_LEN, NUM_HEADS, HEAD_DIM), cos_t, sin_t).astype(jnp.bfloat16)
    k_rot = apply_rope(jnp.dot(normed, w_k, preferred_element_type=jnp.float32).reshape(SEQ_LEN, NUM_KV_HEADS, HEAD_DIM), cos_t, sin_t).astype(jnp.bfloat16)
    v_all = jnp.dot(normed, w_v, preferred_element_type=jnp.float32).astype(jnp.bfloat16).reshape(SEQ_LEN, NUM_KV_HEADS, HEAD_DIM)
    q_grp = q_rot.reshape(NUM_BLOCKS, ROW_BLOCK, NUM_KV_HEADS, GROUP_SIZE, HEAD_DIM)
    k_f32 = k_rot.astype(jnp.float32)
    v_f32 = v_all.astype(jnp.float32)
    block_ids = jnp.arange(NUM_BLOCKS)

    def fwd_block(block_in):
        q_block, block_idx = block_in
        attn_prob = block_probs(q_block.astype(jnp.float32), block_idx * ROW_BLOCK, k_f32)
        prob_bf = attn_prob.astype(jnp.bfloat16).astype(jnp.float32)
        return jnp.einsum('grqk,kgd->qgrd', prob_bf, v_f32).astype(jnp.bfloat16)

    o_grp = lax.map(fwd_block, (q_grp, block_ids))
    o_tok = o_grp.reshape(SEQ_LEN, NUM_HEADS * HEAD_DIM)
    attn_out = jnp.dot(o_tok, w_o, preferred_element_type=jnp.float32).astype(jnp.bfloat16)
    d_o = jnp.dot(d_attn, w_o.T, preferred_element_type=jnp.float32).astype(jnp.bfloat16)
    dw_o = jnp.dot(o_tok.T, d_attn, preferred_element_type=jnp.float32)
    do_grp = d_o.reshape(NUM_BLOCKS, ROW_BLOCK, NUM_KV_HEADS, GROUP_SIZE, HEAD_DIM)

    def bwd_block(carry, block_in):
        dk_acc, dv_acc = carry
        q_block, do_block, block_idx = block_in
        q_f32 = q_block.astype(jnp.float32)
        do_f32 = do_block.astype(jnp.float32)
        attn_prob = block_probs(q_f32, block_idx * ROW_BLOCK, k_f32)
        prob_bf = attn_prob.astype(jnp.bfloat16).astype(jnp.float32)
        d_prob = jnp.einsum('qgrd,kgd->grqk', do_f32, v_f32)
        row_dot = jnp.sum(attn_prob * d_prob, axis=-1, keepdims=True)
        d_score = (attn_prob * (d_prob - row_dot) * SCORE_SCALE).astype(jnp.bfloat16).astype(jnp.float32)
        dq_block = jnp.einsum('grqk,kgd->qgrd', d_score, k_f32).astype(jnp.bfloat16)
        dk_acc = dk_acc + jnp.einsum('grqk,qgrd->kgd', d_score, q_f32)
        dv_acc = dv_acc + jnp.einsum('grqk,qgrd->kgd', prob_bf, do_f32)
        return (dk_acc, dv_acc), dq_block

    zero_acc = jnp.zeros((SEQ_LEN, NUM_KV_HEADS, HEAD_DIM), jnp.float32)
    kv_sums, dq_grp = lax.scan(bwd_block, (zero_acc, zero_acc), (q_grp, do_grp, block_ids))
    dk_bf = kv_sums[0].astype(jnp.bfloat16)
    dv_bf = kv_sums[1].astype(jnp.bfloat16)
    g_q = apply_rope(dq_grp.reshape(SEQ_LEN, NUM_HEADS, HEAD_DIM).astype(jnp.float32), cos_t, -sin_t).astype(jnp.bfloat16).reshape(SEQ_LEN, NUM_HEADS * HEAD_DIM)
    g_k = apply_rope(dk_bf.astype(jnp.float32), cos_t, -sin_t).astype(jnp.bfloat16).reshape(SEQ_LEN, NUM_KV_HEADS * HEAD_DIM)
    g_v = dv_bf.reshape(SEQ_LEN, NUM_KV_HEADS * HEAD_DIM)
    d_normed = (jnp.dot(g_q, w_q.T, preferred_element_type=jnp.float32)
                + jnp.dot(g_k, w_k.T, preferred_element_type=jnp.float32)
                + jnp.dot(g_v, w_v.T, preferred_element_type=jnp.float32))
    dw_q = jnp.dot(normed.T, g_q, preferred_element_type=jnp.float32)
    dw_k = jnp.dot(normed.T, g_k, preferred_element_type=jnp.float32)
    dw_v = jnp.dot(normed.T, g_v, preferred_element_type=jnp.float32)
    d_hid, d_lnw = norm_vjp(d_normed)
    return (attn_out, d_hid.astype(jnp.bfloat16), d_lnw.astype(jnp.bfloat16), dw_q.astype(jnp.bfloat16),
            dw_k.astype(jnp.bfloat16), dw_v.astype(jnp.bfloat16), dw_o.astype(jnp.bfloat16))
```

```python
import functools
import math
import jax
import jax.numpy as jnp
from jax import lax
from jax.experimental import pallas as pl
from jax.experimental.pallas import tpu as pltpu
from jax.sharding import PartitionSpec as P

HEAD_DIM = 128
LN_EPS = 1e-5
ROPE_BASE = 10000.0
SCALE = HEAD_DIM ** -0.5
LOG2E = math.log2(math.e)
C2 = SCALE * LOG2E
NEG = -1e30
VLIM = 56 * 1024 * 1024
F32 = jnp.float32
BF16 = jnp.bfloat16


def norm_f32(hid_f32, weight_f32):
    mean_val = jnp.mean(hid_f32, axis=-1, keepdims=True)
    centered = hid_f32 - mean_val
    var_val = jnp.mean(centered * centered, axis=-1, keepdims=True)
    return centered * lax.rsqrt(var_val + LN_EPS) * weight_f32


def rope_tables(positions):
    lane = jnp.arange(HEAD_DIM)
    inv_freq = ROPE_BASE ** (-(lane - lane % 2).astype(F32) / HEAD_DIM)
    angles = positions.astype(F32)[:, None] * inv_freq[None, :]
    sign = jnp.where(lane % 2 == 0, -1.0, 1.0).astype(F32)
    return jnp.cos(angles), jnp.sin(angles) * sign[None, :]


def swap_pairs(val):
    lane = lax.broadcasted_iota(jnp.int32, val.shape, 1)
    return jnp.where(lane % 2 == 0, pltpu.roll(val, HEAD_DIM - 1, 1), pltpu.roll(val, 1, 1))


def rotate(val, cos_t, sin_t):
    return val * cos_t + swap_pairs(val) * sin_t


def dot_f32(lhs, rhs):
    return jnp.dot(lhs, rhs, preferred_element_type=F32)


def proj_kernel(heads, h_ref, w_ref, cos_ref, sin_ref, q_ref, k_ref, v_ref, qt_ref, kt_ref, vt_ref):
    cos_t, sin_t = cos_ref[...], sin_ref[...]
    width = heads * HEAD_DIM
    for idx, (out, out_t) in enumerate(((q_ref, qt_ref), (k_ref, kt_ref), (v_ref, vt_ref))):
        prod = dot_f32(h_ref[...], w_ref[:, idx * width:(idx + 1) * width])
        for n in range(heads):
            val = prod[:, n * HEAD_DIM:(n + 1) * HEAD_DIM]
            if idx < 2:
                val = rotate(val, cos_t, sin_t)
            out[n] = val.astype(BF16)
            out_t[n] = val.T.astype(BF16)


def project(h_all, w_cat, cos_t, sin_t, heads):
    rows, feat = h_all.shape
    width = w_cat.shape[1]
    bm = math.gcd(rows, 512)
    tok = pl.BlockSpec((heads, bm, HEAD_DIM), lambda i: (0, i, 0))
    tr = pl.BlockSpec((heads, HEAD_DIM, bm), lambda i: (0, 0, i))
    tab = pl.BlockSpec((bm, HEAD_DIM), lambda i: (i, 0))
    s_tok = jax.ShapeDtypeStruct((heads, rows, HEAD_DIM), BF16)
    s_tr = jax.ShapeDtypeStruct((heads, HEAD_DIM, rows), BF16)
    return pl.pallas_call(
        functools.partial(proj_kernel, heads), grid=(rows // bm,), name='qkv_proj',
        in_specs=[pl.BlockSpec((bm, feat), lambda i: (i, 0)), pl.BlockSpec((feat, width), lambda i: (0, 0)), tab, tab],
        out_specs=[tok] * 3 + [tr] * 3, out_shape=[s_tok] * 3 + [s_tr] * 3,
        compiler_params=pltpu.CompilerParams(vmem_limit_bytes=VLIM),
        cost_estimate=pl.CostEstimate(flops=2 * rows * feat * width, bytes_accessed=2 * rows * feat, transcendentals=0),
    )(h_all, w_cat, cos_t, sin_t)


def fwd_kernel(blk, k_ref, qt_ref, vt_ref, o_ref, ot_ref, lse_ref, acc_ref):
    qi = pl.program_id(1)
    qt = qt_ref[0]
    acc_ref[...] = jnp.zeros_like(acc_ref)

    def chunk(j, carry, masked):
        m_old, l_old = carry
        start = pl.multiple_of(j * blk, blk)
        s_t = dot_f32(k_ref[0, pl.ds(start, blk), :], qt)
        if masked:
            key = lax.broadcasted_iota(jnp.int32, s_t.shape, 0)
            qry = lax.broadcasted_iota(jnp.int32, s_t.shape, 1)
            s_t = jnp.where(key <= qry, s_t, NEG)
        m_new = jnp.maximum(m_old, jnp.max(s_t, axis=0, keepdims=True) * C2)
        p_t = jnp.exp2(s_t * C2 - m_new)
        alpha = jnp.exp2(m_old - m_new)
        l_new = l_old * alpha + jnp.sum(p_t, axis=0, keepdims=True)
        acc_ref[...] = acc_ref[...] * alpha + dot_f32(vt_ref[0, :, pl.ds(start, blk)], p_t.astype(BF16))
        return m_new, l_new

    init = (jnp.full((1, blk), NEG, F32), jnp.zeros((1, blk), F32))
    carry = lax.fori_loop(0, qi, lambda j, c: chunk(j, c, False), init)
    m_fin, l_fin = chunk(qi, carry, True)
    o_t = acc_ref[...] / l_fin
    ot_ref[0] = o_t
    o_ref[...] = o_t.T.astype(BF16)
    lse_ref[0] = m_fin + jnp.log2(l_fin)


def attn_fwd(k, q_t, v_t):
    heads, rows, _ = k.shape
    blk = math.gcd(rows, 512)
    full = pl.BlockSpec((1, rows, HEAD_DIM), lambda n, i: (n, 0, 0))
    full_t = pl.BlockSpec((1, HEAD_DIM, rows), lambda n, i: (n, 0, 0))
    blk_t = pl.BlockSpec((1, HEAD_DIM, blk), lambda n, i: (n, 0, i))
    return pl.pallas_call(
        functools.partial(fwd_kernel, blk), grid=(heads, rows // blk), name='attn_fwd',
        in_specs=[full, blk_t, full_t],
        out_specs=[pl.BlockSpec((blk, HEAD_DIM), lambda n, i: (i, n)), blk_t,
                   pl.BlockSpec((1, 1, blk), lambda n, i: (n, 0, i))],
        out_shape=[jax.ShapeDtypeStruct((rows, heads * HEAD_DIM), BF16),
                   jax.ShapeDtypeStruct((heads, HEAD_DIM, rows), F32),
                   jax.ShapeDtypeStruct((heads, 1, rows), F32)],
        scratch_shapes=[pltpu.VMEM((HEAD_DIM, blk), F32)],
        compiler_params=pltpu.CompilerParams(vmem_limit_bytes=VLIM),
        cost_estimate=pl.CostEstimate(flops=4 * heads * rows * rows * HEAD_DIM, bytes_accessed=8 * heads * rows * HEAD_DIM,
                                      transcendentals=heads * rows * rows // 2),
    )(k, q_t, v_t)


def do_kernel(heads, g_ref, wo_ref, ot_ref, do_ref, dot_ref, dsum_ref):
    prod = lax.dot_general(g_ref[...], wo_ref[...], (((1,), (1,)), ((), ())), preferred_element_type=F32)
    for n in range(heads):
        val = prod[:, n * HEAD_DIM:(n + 1) * HEAD_DIM].astype(BF16)
        val_t = val.astype(F32).T
        do_ref[n] = val
        dot_ref[n] = val_t.astype(BF16)
        dsum_ref[n] = jnp.sum(val_t * ot_ref[n], axis=0, keepdims=True)


def project_do(g_all, wo_rows, o_t, heads):
    rows, feat = g_all.shape
    width = wo_rows.shape[0]
    bm = math.gcd(rows, 512)
    tok = pl.BlockSpec((heads, bm, HEAD_DIM), lambda i: (0, i, 0))
    tr = pl.BlockSpec((heads, HEAD_DIM, bm), lambda i: (0, 0, i))
    return pl.pallas_call(
        functools.partial(do_kernel, heads), grid=(rows // bm,), name='do_proj',
        in_specs=[pl.BlockSpec((bm, feat), lambda i: (i, 0)), pl.BlockSpec((width, feat), lambda i: (0, 0)), tr],
        out_specs=[tok, tr, pl.BlockSpec((heads, 1, bm), lambda i: (0, 0, i))],
        out_shape=[jax.ShapeDtypeStruct((heads, rows, HEAD_DIM), BF16), jax.ShapeDtypeStruct((heads, HEAD_DIM, rows), BF16),
                   jax.ShapeDtypeStruct((heads, 1, rows), F32)],
        compiler_params=pltpu.CompilerParams(vmem_limit_bytes=VLIM),
        cost_estimate=pl.CostEstimate(flops=2 * rows * feat * width, bytes_accessed=2 * rows * feat, transcendentals=0),
    )(g_all, wo_rows, o_t)


def bwd_kernel(blk, n_blk, k_ref, v_ref, kt_ref, q_ref, qt_ref, do_ref, dot_ref, lse_ref, dsum_ref, cos_ref, sin_ref,
               gq_ref, gk_ref, gv_ref, dqt_ref, dk_ref, dv_ref):
    kj = pl.program_id(0)
    k_blk, v_blk, kt_blk = k_ref[0], v_ref[0], kt_ref[0]

    @pl.when(kj == 0)
    def _():
        dqt_ref[...] = jnp.zeros_like(dqt_ref)

    def chunk(i, masked):
        start = pl.multiple_of(i * blk, blk)
        cols = pl.ds(start, blk)
        p_t = jnp.exp2(dot_f32(k_blk, qt_ref[0, :, cols]) * C2 - lse_ref[0, :, cols])
        if masked:
            key = lax.broadcasted_iota(jnp.int32, p_t.shape, 0)
            qry = lax.broadcasted_iota(jnp.int32, p_t.shape, 1)
            p_t = jnp.where(key <= qry, p_t, 0.0)
        dp_t = dot_f32(v_blk, dot_ref[0, :, cols])
        ds_t = (p_t * ((dp_t - dsum_ref[0, :, cols]) * SCALE)).astype(BF16)
        dv_new = dot_f32(p_t.astype(BF16), do_ref[0, cols, :])
        dk_new = dot_f32(ds_t, q_ref[0, cols, :])
        if masked:
            dv_ref[...] = dv_new
            dk_ref[...] = dk_new
        else:
            dv_ref[...] += dv_new
            dk_ref[...] += dk_new
        dqt_ref[:, cols] += dot_f32(kt_blk, ds_t)

    chunk(kj, True)
    lax.fori_loop(kj + 1, n_blk, lambda i, c: (chunk(i, False), c)[1], 0)
    cos_t, sin_t = cos_ref[...], -sin_ref[...]
    own = pl.ds(pl.multiple_of(kj * blk, blk), blk)
    d_q = dqt_ref[:, own].T.astype(BF16).astype(F32)
    gq_ref[...] = rotate(d_q, cos_t, sin_t).astype(BF16)
    gk_ref[...] = rotate(dk_ref[...].astype(BF16).astype(F32), cos_t, sin_t).astype(BF16)
    gv_ref[...] = dv_ref[...].astype(BF16)


def attn_bwd(n, k, v, k_t, q, q_t, d_o, d_ot, lse, dsum, cos_t, sin_t):
    heads, rows, _ = k.shape
    blk = math.gcd(rows, 512)
    n_blk = rows // blk
    blk_tok = pl.BlockSpec((1, blk, HEAD_DIM), lambda j: (n, j, 0))
    blk_tr = pl.BlockSpec((1, HEAD_DIM, blk), lambda j: (n, 0, j))
    full = pl.BlockSpec((1, rows, HEAD_DIM), lambda j: (n, 0, 0))
    full_t = pl.BlockSpec((1, HEAD_DIM, rows), lambda j: (n, 0, 0))
    vec = pl.BlockSpec((1, 1, rows), lambda j: (n, 0, 0))
    tab = pl.BlockSpec((blk, HEAD_DIM), lambda j: (j, 0))
    return pl.pallas_call(
        functools.partial(bwd_kernel, blk, n_blk), grid=(n_blk,), name='attn_bwd',
        in_specs=[blk_tok, blk_tok, blk_tr, full, full_t, full, full_t, vec, vec, tab, tab],
        out_specs=[tab] * 3, out_shape=[jax.ShapeDtypeStruct((rows, HEAD_DIM), BF16)] * 3,
        scratch_shapes=[pltpu.VMEM((HEAD_DIM, rows), F32), pltpu.VMEM((blk, HEAD_DIM), F32), pltpu.VMEM((blk, HEAD_DIM), F32)],
        compiler_params=pltpu.CompilerParams(vmem_limit_bytes=VLIM),
        cost_estimate=pl.CostEstimate(flops=10 * rows * rows * HEAD_DIM, bytes_accessed=20 * rows * HEAD_DIM,
                                      transcendentals=rows * rows // 2),
    )(k, v, k_t, q, q_t, d_o, d_ot, lse, dsum, cos_t, sin_t)


def solution(mesh):
    sp_size = mesh.shape['sp']
    row_spec = P(('dp', 'sp'), None)
    pos_spec = P(('dp', 'sp'))
    full_spec = P(None, None)
    grad_spec = P('dp', None)

    def local_step(hidden, positions, d_attn, ln_weight, w_q, w_k, w_v, w_o):
        width = w_q.shape[1] // sp_size
        heads = width // HEAD_DIM
        me = lax.axis_index('sp')
        normed32, norm_vjp = jax.vjp(norm_f32, hidden.astype(F32), ln_weight.astype(F32))
        normed = normed32.astype(BF16)
        pos_all = lax.all_gather(positions, 'sp', axis=0, tiled=True)
        h_all = lax.all_gather(normed, 'sp', axis=0, tiled=True)
        g_dep, h_all = lax.optimization_barrier((d_attn, h_all))
        g_all = lax.all_gather(g_dep, 'sp', axis=0, tiled=True)
        cos_t, sin_t = rope_tables(pos_all)
        own = lambda w: lax.dynamic_slice_in_dim(w, me * width, width, 1)
        w_cat = jnp.concatenate([own(w_q), own(w_k), own(w_v)], axis=1)
        wo_rows = lax.dynamic_slice_in_dim(w_o, me * width, width, 0)
        q, k, v, q_t, k_t, v_t = project(h_all, w_cat, cos_t, sin_t, heads)
        o_tok, o_t, lse = attn_fwd(k, q_t, v_t)
        d_o, d_ot, dsum = project_do(g_all, wo_rows, o_t, heads)

        def to_owner(val):
            return lax.all_to_all(val, 'sp', 0, 1, tiled=True)

        def gather(grad, axis):
            return lax.all_gather(grad, 'sp', axis=axis, tiled=True)

        o_own = to_owner(o_tok)
        attn_out = dot_f32(o_own, w_o).astype(BF16)
        dw_o = gather(jnp.einsum('te,td->ed', o_tok, g_all, preferred_element_type=F32).astype(BF16), 0)
        parts = [attn_bwd(n, k, v, k_t, q, q_t, d_o, d_ot, lse, dsum, cos_t, sin_t) for n in range(heads)]
        grads = []
        d_normed = 0.0
        for idx, w in enumerate((w_q, w_k, w_v)):
            g_tok = jnp.concatenate([part[idx] for part in parts], axis=1)
            d_w = jnp.einsum('td,te->de', h_all, g_tok, preferred_element_type=F32).astype(BF16)
            grads.append(gather(d_w, 1))
            d_normed = d_normed + jnp.einsum('te,de->td', to_owner(g_tok), w, preferred_element_type=F32)
        d_hid, d_lnw = norm_vjp(d_normed)
        d_lnw = lax.psum(d_lnw, 'sp')
        return (attn_out, d_hid.astype(BF16), d_lnw.astype(BF16), grads[0], grads[1], grads[2], dw_o)

    return jax.shard_map(local_step, mesh=mesh,
                         in_specs=(row_spec, pos_spec, row_spec, P(None), full_spec, full_spec, full_spec, full_spec),
                         out_specs=(row_spec, row_spec, P('dp'), grad_spec, grad_spec, grad_spec, grad_spec),
                         check_vma=False)
```

```python
import functools
import math
import jax
import jax.numpy as jnp
from jax import lax
from jax.experimental import pallas as pl
from jax.experimental.layout import Layout, with_layout_constraint
from jax.experimental.pallas import tpu as pltpu
from jax.sharding import PartitionSpec as P

HEAD_DIM = 128
LN_EPS = 1e-5
ROPE_BASE = 10000.0
SCALE = HEAD_DIM ** -0.5
LOG2E = math.log2(math.e)
C2 = SCALE * LOG2E
NEG = -1e30
VLIM = 56 * 1024 * 1024
F32 = jnp.float32
BF16 = jnp.bfloat16


def norm_f32(hid_f32, weight_f32):
    mean_val = jnp.mean(hid_f32, axis=-1, keepdims=True)
    centered = hid_f32 - mean_val
    var_val = jnp.mean(centered * centered, axis=-1, keepdims=True)
    return centered * lax.rsqrt(var_val + LN_EPS) * weight_f32


def norm_kernel(x_ref, w_ref, out_ref):
    out_ref[...] = norm_f32(x_ref[...].astype(F32), w_ref[...].astype(F32)).astype(BF16)


def layer_norm(hidden, weight):
    rows, feat = hidden.shape
    bm = math.gcd(rows, 256)
    spec = pl.BlockSpec((bm, feat), lambda i: (i, 0))
    return pl.pallas_call(
        norm_kernel, grid=(rows // bm,), name='layer_norm',
        in_specs=[spec, pl.BlockSpec((1, feat), lambda i: (0, 0))], out_specs=spec,
        out_shape=jax.ShapeDtypeStruct((rows, feat), BF16),
        cost_estimate=pl.CostEstimate(flops=10 * rows * feat, bytes_accessed=4 * rows * feat, transcendentals=rows),
    )(hidden, weight[None, :])


def rope_tables(positions):
    lane = jnp.arange(HEAD_DIM)
    inv_freq = ROPE_BASE ** (-(lane - lane % 2).astype(F32) / HEAD_DIM)
    angles = positions.astype(F32)[:, None] * inv_freq[None, :]
    sign = jnp.where(lane % 2 == 0, -1.0, 1.0).astype(F32)
    return jnp.cos(angles), jnp.sin(angles) * sign[None, :]


def swap_pairs(val):
    lane = lax.broadcasted_iota(jnp.int32, val.shape, 1)
    return jnp.where(lane % 2 == 0, pltpu.roll(val, HEAD_DIM - 1, 1), pltpu.roll(val, 1, 1))


def rotate(val, cos_t, sin_t):
    return val * cos_t + swap_pairs(val) * sin_t


def dot_f32(lhs, rhs):
    return jnp.dot(lhs, rhs, preferred_element_type=F32)


def proj_kernel(heads, h_ref, w_ref, cos_ref, sin_ref, q_ref, k_ref, v_ref, qt_ref, kt_ref, vt_ref):
    cos_t, sin_t = cos_ref[...], sin_ref[...]
    width = heads * HEAD_DIM
    for idx, (out, out_t) in enumerate(((q_ref, qt_ref), (k_ref, kt_ref), (v_ref, vt_ref))):
        prod = dot_f32(h_ref[...], w_ref[:, idx * width:(idx + 1) * width])
        for n in range(heads):
            val = prod[:, n * HEAD_DIM:(n + 1) * HEAD_DIM]
            if idx < 2:
                val = rotate(val, cos_t, sin_t)
            val = val.astype(BF16)
            out[n] = val
            out_t[n] = val.T


def project(h_all, w_cat, cos_t, sin_t, heads):
    rows, feat = h_all.shape
    width = w_cat.shape[1]
    bm = math.gcd(rows, 512)
    tok = pl.BlockSpec((heads, bm, HEAD_DIM), lambda i: (0, i, 0))
    tr = pl.BlockSpec((heads, HEAD_DIM, bm), lambda i: (0, 0, i))
    tab = pl.BlockSpec((bm, HEAD_DIM), lambda i: (i, 0))
    s_tok = jax.ShapeDtypeStruct((heads, rows, HEAD_DIM), BF16)
    s_tr = jax.ShapeDtypeStruct((heads, HEAD_DIM, rows), BF16)
    return pl.pallas_call(
        functools.partial(proj_kernel, heads), grid=(rows // bm,), name='qkv_proj',
        in_specs=[pl.BlockSpec((bm, feat), lambda i: (i, 0)), pl.BlockSpec((feat, width), lambda i: (0, 0)), tab, tab],
        out_specs=[tok] * 3 + [tr] * 3, out_shape=[s_tok] * 3 + [s_tr] * 3,
        compiler_params=pltpu.CompilerParams(vmem_limit_bytes=VLIM),
        cost_estimate=pl.CostEstimate(flops=2 * rows * feat * width, bytes_accessed=2 * rows * feat, transcendentals=0),
    )(h_all, w_cat, cos_t, sin_t)


def fwd_kernel(blk, heads, k_ref, qt_ref, vt_ref, o_ref, ot_ref, lse_ref, acc_ref):
    qi = pl.program_id(0)
    acc_ref[...] = jnp.zeros_like(acc_ref)

    def chunk(j, carry, masked):
        start = pl.multiple_of(j * blk, blk)
        scores = [dot_f32(k_ref[n, pl.ds(start, blk), :], qt_ref[n]) for n in range(heads)]
        if masked:
            key = lax.broadcasted_iota(jnp.int32, (blk, blk), 0)
            qry = lax.broadcasted_iota(jnp.int32, (blk, blk), 1)
            scores = [jnp.where(key <= qry, s_t, NEG) for s_t in scores]
        out = []
        for n in range(heads):
            m_old, l_old = carry[n]
            s_t = scores[n]
            m_new = jnp.maximum(m_old, jnp.max(s_t, axis=0, keepdims=True) * C2)
            p_t = jnp.exp2(s_t * C2 - m_new)
            alpha = jnp.exp2(m_old - m_new)
            l_new = l_old * alpha + jnp.sum(p_t, axis=0, keepdims=True)
            acc_ref[n] = acc_ref[n] * alpha + dot_f32(vt_ref[n, :, pl.ds(start, blk)], p_t.astype(BF16))
            out.append((m_new, l_new))
        return tuple(out)

    init = tuple((jnp.full((1, blk), NEG, F32), jnp.zeros((1, blk), F32)) for _ in range(heads))
    carry = lax.fori_loop(0, qi, lambda j, c: chunk(j, c, False), init)
    carry = chunk(qi, carry, True)
    for n in range(heads):
        m_fin, l_fin = carry[n]
        o_t = acc_ref[n] / l_fin
        ot_ref[n] = o_t
        o_ref[:, n * HEAD_DIM:(n + 1) * HEAD_DIM] = o_t.T.astype(BF16)
        lse_ref[n] = m_fin + jnp.log2(l_fin)


def attn_fwd(k, q_t, v_t):
    heads, rows, _ = k.shape
    blk = math.gcd(rows, 768)
    full = pl.BlockSpec((heads, rows, HEAD_DIM), lambda i: (0, 0, 0))
    full_t = pl.BlockSpec((heads, HEAD_DIM, rows), lambda i: (0, 0, 0))
    blk_t = pl.BlockSpec((heads, HEAD_DIM, blk), lambda i: (0, 0, i))
    return pl.pallas_call(
        functools.partial(fwd_kernel, blk, heads), grid=(rows // blk,), name='attn_fwd',
        in_specs=[full, blk_t, full_t],
        out_specs=[pl.BlockSpec((blk, heads * HEAD_DIM), lambda i: (i, 0)), blk_t,
                   pl.BlockSpec((heads, 1, blk), lambda i: (0, 0, i))],
        out_shape=[jax.ShapeDtypeStruct((rows, heads * HEAD_DIM), BF16),
                   jax.ShapeDtypeStruct((heads, HEAD_DIM, rows), F32),
                   jax.ShapeDtypeStruct((heads, 1, rows), F32)],
        scratch_shapes=[pltpu.VMEM((heads, HEAD_DIM, blk), F32)],
        compiler_params=pltpu.CompilerParams(vmem_limit_bytes=VLIM),
        cost_estimate=pl.CostEstimate(flops=4 * heads * rows * rows * HEAD_DIM, bytes_accessed=8 * heads * rows * HEAD_DIM,
                                      transcendentals=heads * rows * rows // 2),
    )(k, q_t, v_t)


def do_kernel(heads, g_ref, wo_ref, ot_ref, do_ref, dot_ref, dsum_ref, dwo_ref, acc_ref):
    step = pl.program_id(0)

    @pl.when(step == 0)
    def _():
        acc_ref[...] = jnp.zeros_like(acc_ref)

    prod = dot_f32(g_ref[...], wo_ref[...])
    for n in range(heads):
        own = slice(n * HEAD_DIM, (n + 1) * HEAD_DIM)
        val = prod[:, own].astype(BF16)
        val_t = val.T
        o_t = ot_ref[n]
        do_ref[n] = val
        dot_ref[n] = val_t
        dsum_ref[n] = jnp.sum(val_t.astype(F32) * o_t, axis=0, keepdims=True)
        acc_ref[own, :] += dot_f32(o_t.astype(BF16), g_ref[...])

    @pl.when(step == pl.num_programs(0) - 1)
    def _():
        dwo_ref[...] = acc_ref[...].astype(BF16)


def project_do(g_all, wo_cols, o_t, heads):
    rows, feat = g_all.shape
    width = wo_cols.shape[1]
    bm = math.gcd(rows, 1024)
    tok = pl.BlockSpec((heads, bm, HEAD_DIM), lambda i: (0, i, 0))
    tr = pl.BlockSpec((heads, HEAD_DIM, bm), lambda i: (0, 0, i))
    return pl.pallas_call(
        functools.partial(do_kernel, heads), grid=(rows // bm,), name='do_dwo',
        in_specs=[pl.BlockSpec((bm, feat), lambda i: (i, 0)), pl.BlockSpec((feat, width), lambda i: (0, 0)), tr],
        out_specs=[tok, tr, pl.BlockSpec((heads, 1, bm), lambda i: (0, 0, i)), pl.BlockSpec((width, feat), lambda i: (0, 0))],
        out_shape=[jax.ShapeDtypeStruct((heads, rows, HEAD_DIM), BF16), jax.ShapeDtypeStruct((heads, HEAD_DIM, rows), BF16),
                   jax.ShapeDtypeStruct((heads, 1, rows), F32), jax.ShapeDtypeStruct((width, feat), BF16)],
        scratch_shapes=[pltpu.VMEM((width, feat), F32)],
        compiler_params=pltpu.CompilerParams(vmem_limit_bytes=VLIM),
        cost_estimate=pl.CostEstimate(flops=4 * rows * feat * width, bytes_accessed=2 * rows * feat, transcendentals=0),
    )(g_all, wo_cols, o_t)


def bwd_kernel(blk, n_blk, k_ref, v_ref, kt_ref, q_ref, qt_ref, do_ref, dot_ref, lse_ref, dsum_ref, cos_ref, sin_ref,
               g_ref, dqt_ref, dk_ref, dv_ref):
    kj = pl.program_id(0)
    half = blk // 2

    @pl.when(kj == 0)
    def _():
        dqt_ref[...] = jnp.zeros_like(dqt_ref)

    def tile(k_lo, k_num, q_start, q_num, masked, first):
        keys = slice(k_lo, k_lo + k_num)
        cols = pl.ds(q_start, q_num)
        p_t = jnp.exp2(dot_f32(k_ref[0, keys, :], qt_ref[0, :, cols]) * C2 - lse_ref[0, :, cols])
        if masked:
            key = lax.broadcasted_iota(jnp.int32, p_t.shape, 0)
            qry = lax.broadcasted_iota(jnp.int32, p_t.shape, 1)
            p_t = jnp.where(key <= qry, p_t, 0.0)
        dp_t = dot_f32(v_ref[0, keys, :], dot_ref[0, :, cols])
        ds_t = (p_t * ((dp_t - dsum_ref[0, :, cols]) * SCALE)).astype(BF16)
        dv_new = dot_f32(p_t.astype(BF16), do_ref[0, cols, :])
        dk_new = dot_f32(ds_t, q_ref[0, cols, :])
        if first:
            dv_ref[keys, :] = dv_new
            dk_ref[keys, :] = dk_new
        else:
            dv_ref[keys, :] += dv_new
            dk_ref[keys, :] += dk_new
        dqt_ref[:, cols] += dot_f32(kt_ref[0, :, keys], ds_t)

    base = pl.multiple_of(kj * blk, blk)
    tile(0, half, base, half, True, True)
    tile(half, half, base + half, half, True, True)
    tile(0, half, base + half, half, False, False)

    def body(i, carry):
        tile(0, blk, pl.multiple_of(i * blk, blk), blk, False, False)
        return carry

    lax.fori_loop(kj + 1, n_blk, body, 0)
    cos_t, sin_t = cos_ref[...], -sin_ref[...]
    d_q = dqt_ref[:, pl.ds(base, blk)].T.astype(BF16).astype(F32)
    g_ref[:, :HEAD_DIM] = rotate(d_q, cos_t, sin_t).astype(BF16)
    g_ref[:, HEAD_DIM:2 * HEAD_DIM] = rotate(dk_ref[...].astype(BF16).astype(F32), cos_t, sin_t).astype(BF16)
    g_ref[:, 2 * HEAD_DIM:] = dv_ref[...].astype(BF16)


def attn_bwd(n, k, v, k_t, q, q_t, d_o, d_ot, lse, dsum, cos_t, sin_t):
    _, rows, _ = k.shape
    blk = math.gcd(rows, 1024)
    n_blk = rows // blk
    blk_tok = pl.BlockSpec((1, blk, HEAD_DIM), lambda j: (n, j, 0))
    blk_tr = pl.BlockSpec((1, HEAD_DIM, blk), lambda j: (n, 0, j))
    full = pl.BlockSpec((1, rows, HEAD_DIM), lambda j: (n, 0, 0))
    full_t = pl.BlockSpec((1, HEAD_DIM, rows), lambda j: (n, 0, 0))
    vec = pl.BlockSpec((1, 1, rows), lambda j: (n, 0, 0))
    tab = pl.BlockSpec((blk, HEAD_DIM), lambda j: (j, 0))
    return pl.pallas_call(
        functools.partial(bwd_kernel, blk, n_blk), grid=(n_blk,), name='attn_bwd',
        in_specs=[blk_tok, blk_tok, blk_tr, full, full_t, full, full_t, vec, vec, tab, tab],
        out_specs=pl.BlockSpec((blk, 3 * HEAD_DIM), lambda j: (j, 0)),
        out_shape=jax.ShapeDtypeStruct((rows, 3 * HEAD_DIM), BF16),
        scratch_shapes=[pltpu.VMEM((HEAD_DIM, rows), F32), pltpu.VMEM((blk, HEAD_DIM), F32), pltpu.VMEM((blk, HEAD_DIM), F32)],
        compiler_params=pltpu.CompilerParams(vmem_limit_bytes=VLIM),
        cost_estimate=pl.CostEstimate(flops=10 * rows * rows * HEAD_DIM, bytes_accessed=20 * rows * HEAD_DIM,
                                      transcendentals=rows * rows // 2),
    )(k, v, k_t, q, q_t, d_o, d_ot, lse, dsum, cos_t, sin_t)


def copy_kernel(a_ref, out_ref):
    out_ref[...] = a_ref[...]


def copy_rows(val):
    rows, feat = val.shape
    spec = pl.BlockSpec((math.gcd(rows, 256), feat), lambda i: (i, 0))
    return pl.pallas_call(
        copy_kernel, grid=(rows // spec.block_shape[0],), name='copy_rows', in_specs=[spec], out_specs=spec,
        out_shape=jax.ShapeDtypeStruct(val.shape, val.dtype),
        cost_estimate=pl.CostEstimate(flops=rows * feat, bytes_accessed=4 * rows * feat, transcendentals=0),
    )(val)


def place_kernel(a_ref, *refs):
    for idx, out in enumerate(refs[-3:]):
        out[...] = a_ref[0, :, idx * HEAD_DIM:(idx + 1) * HEAD_DIM]


def place_slot(n, heads, gathered, grads):
    devs, feat, width = gathered.shape
    spec = pl.BlockSpec((feat, HEAD_DIM), lambda j: (0, j * heads + n))
    shape = jax.ShapeDtypeStruct((feat, devs * heads * HEAD_DIM), BF16)
    return pl.pallas_call(
        place_kernel, grid=(devs,), name='place',
        in_specs=[pl.BlockSpec((1, feat, width), lambda j: (j, 0, 0))] + [pl.BlockSpec(memory_space=pl.ANY)] * len(grads),
        out_specs=[spec] * 3, out_shape=[shape] * 3,
        input_output_aliases={1 + i: i for i in range(len(grads))},
        compiler_params=pltpu.CompilerParams(vmem_limit_bytes=VLIM),
        cost_estimate=pl.CostEstimate(flops=devs * feat * width, bytes_accessed=4 * devs * feat * width, transcendentals=0),
    )(gathered, *grads)


def solution(mesh):
    sp_size = mesh.shape['sp']
    row_spec = P(('dp', 'sp'), None)
    pos_spec = P(('dp', 'sp'))
    full_spec = P(None, None)
    grad_spec = P('dp', None)

    def layer_step(hidden, positions, d_attn, ln_weight, w_q, w_k, w_v, w_o):
        feat, all_width = w_q.shape
        width = all_width // sp_size
        heads = width // HEAD_DIM
        me = lax.axis_index('sp')
        normed = layer_norm(hidden, ln_weight)
        pos_all = lax.all_gather(positions, 'sp', axis=0, tiled=True)
        h_all = lax.all_gather(normed, 'sp', axis=0, tiled=True)
        cos_t, sin_t = rope_tables(pos_all)
        own = lambda w: lax.dynamic_slice_in_dim(w, me * width, width, 1)
        w_cat = jnp.concatenate([own(w_q), own(w_k), own(w_v)], axis=1)
        wo_cols = lax.dynamic_slice_in_dim(w_o, me * width, width, 0).T
        stacked = jnp.stack([w.reshape(feat, sp_size, heads, HEAD_DIM) for w in (w_q, w_k, w_v)], axis=3)
        w_slot = [stacked[:, :, n].reshape(feat, sp_size * 3 * HEAD_DIM) for n in range(heads)]
        h_all, cos_t, sin_t, w_cat, wo_cols, w_slot = lax.optimization_barrier((h_all, cos_t, sin_t, w_cat, wo_cols, w_slot))
        g_dep, h_all = lax.optimization_barrier((d_attn, h_all))
        g_all = lax.all_gather(g_dep, 'sp', axis=0, tiled=True)
        q, k, v, q_t, k_t, v_t = project(h_all, w_cat, cos_t, sin_t, heads)
        o_tok, o_t, lse = attn_fwd(k, q_t, v_t)

        row_major = Layout(major_to_minor=(0, 1, 2))

        def to_owner(val):
            val = with_layout_constraint(val.reshape(sp_size, -1, val.shape[1]), row_major)
            val = with_layout_constraint(lax.all_to_all(val, 'sp', 0, 0, tiled=True), row_major)
            return val.transpose(1, 0, 2).reshape(val.shape[1], -1)

        o_tok, g_all = lax.optimization_barrier((o_tok, g_all))
        o_own = to_owner(o_tok)
        d_o, d_ot, dsum, dw_o = project_do(g_all, wo_cols, o_t, heads)
        dw_o = lax.all_gather(dw_o, 'sp', axis=0, tiled=True)
        dw_o = copy_rows(dw_o)
        attn_out = dot_f32(o_own, w_o).astype(BF16)
        d_ws = []
        d_normed = 0.0
        for n in range(heads):
            g_tok = attn_bwd(n, k, v, k_t, q, q_t, d_o, d_ot, lse, dsum, cos_t, sin_t)
            g_own = to_owner(g_tok)
            d_w = jnp.einsum('td,te->de', h_all, g_tok, preferred_element_type=F32).astype(BF16)
            d_ws.append(lax.all_gather(d_w, 'sp', axis=0))
            d_normed = d_normed + jnp.einsum('te,de->td', g_own, w_slot[n], preferred_element_type=F32)
        grads = ()
        for n in range(heads):
            grads = place_slot(n, heads, d_ws[n], grads)
        norm_vjp = jax.vjp(norm_f32, hidden.astype(F32), ln_weight.astype(F32))[1]
        d_hid, d_lnw = norm_vjp(d_normed)
        d_lnw = lax.psum(d_lnw, 'sp')
        return (attn_out, d_hid.astype(BF16), d_lnw.astype(BF16), grads[0], grads[1], grads[2], dw_o)

    return jax.shard_map(layer_step, mesh=mesh,
                         in_specs=(row_spec, pos_spec, row_spec, P(None), full_spec, full_spec, full_spec, full_spec),
                         out_specs=(row_spec, row_spec, P('dp'), grad_spec, grad_spec, grad_spec, grad_spec),
                         check_vma=False)
```

```python
import functools
import math
import jax
import jax.numpy as jnp
from jax import lax
from jax.experimental import pallas as pl
from jax.experimental.layout import Layout, with_layout_constraint
from jax.experimental.pallas import tpu as pltpu
from jax.sharding import PartitionSpec as P

HEAD_DIM = 128
LN_EPS = 1e-5
ROPE_BASE = 10000.0
SCALE = HEAD_DIM ** -0.5
LOG2E = math.log2(math.e)
C2 = SCALE * LOG2E
NEG = -1e30
VLIM = 56 * 1024 * 1024
F32 = jnp.float32
BF16 = jnp.bfloat16


def norm_f32(hid_f32, weight_f32):
    mean_val = jnp.mean(hid_f32, axis=-1, keepdims=True)
    centered = hid_f32 - mean_val
    var_val = jnp.mean(centered * centered, axis=-1, keepdims=True)
    return centered * lax.rsqrt(var_val + LN_EPS) * weight_f32


def norm_kernel(x_ref, w_ref, out_ref):
    out_ref[...] = norm_f32(x_ref[...].astype(F32), w_ref[...].astype(F32)).astype(BF16)


def layer_norm(hidden, weight):
    rows, feat = hidden.shape
    bm = math.gcd(rows, 256)
    spec = pl.BlockSpec((bm, feat), lambda i: (i, 0))
    return pl.pallas_call(
        norm_kernel, grid=(rows // bm,), name='layer_norm',
        in_specs=[spec, pl.BlockSpec((1, feat), lambda i: (0, 0))], out_specs=spec,
        out_shape=jax.ShapeDtypeStruct((rows, feat), BF16),
        cost_estimate=pl.CostEstimate(flops=10 * rows * feat, bytes_accessed=4 * rows * feat, transcendentals=rows),
    )(hidden, weight[None, :])


def gather_kernel(h_ref, pos_ref, all_ref, pos_all_ref, send, recv, psend, precv, lsem):
    me = lax.axis_index('sp')
    rows = h_ref.shape[0]
    half = rows // 2
    core, x_pos, y_pos = lax.rem(me, 2), lax.rem(me // 2, 2), me // 4
    d_x, d_y, d_c = 2 - 4 * x_pos, 4 - 8 * y_pos, 1 - 2 * core
    x_nbr, y_nbr, c_nbr = me + d_x, me + d_y, me + d_c
    diag = me + d_x + d_y

    barrier = pltpu.get_barrier_semaphore()
    for r in range(1, 8):
        pl.semaphore_signal(barrier, inc=1, device_id={'sp': lax.rem(me + r, 8)}, device_id_type=pl.DeviceIdType.MESH)
    pl.semaphore_wait(barrier, 7)

    def region(owner, part):
        return all_ref.at[pl.ds(pl.multiple_of(owner * rows + part * half, half), half)]

    def copy(k, src, owner, part, dst):
        return pltpu.make_async_remote_copy(src_ref=src, dst_ref=region(owner, part), send_sem=send.at[k], recv_sem=recv.at[k],
                                            device_id={'sp': dst}, device_id_type=pl.DeviceIdType.MESH)

    def own(part):
        return h_ref.at[pl.ds(part * half, half)]

    pos_copies = []
    for r in range(1, 8):
        cp = pltpu.make_async_remote_copy(src_ref=pos_ref, dst_ref=pos_all_ref.at[me], send_sem=psend.at[r - 1], recv_sem=precv.at[r - 1],
                                          device_id={'sp': lax.rem(me + r, 8)}, device_id_type=pl.DeviceIdType.MESH)
        cp.start()
        pos_copies.append(cp)
    sends = {}

    def start(k, src, owner, part, dst):
        sends[k] = copy(k, src, owner, part, dst)
        sends[k].start()

    def arrived(k, owner, part):
        copy(k, region(owner, part), owner, part, me).wait_recv()

    start(0, own(0), me, 0, x_nbr)
    start(3, own(1), me, 1, y_nbr)
    start(1, own(1), me, 1, x_nbr)
    start(2, own(0), me, 0, y_nbr)
    start(4, own(0), me, 0, c_nbr)
    start(5, own(1), me, 1, c_nbr)
    local = [pltpu.make_async_copy(h_ref, all_ref.at[pl.ds(pl.multiple_of(me * rows, rows), rows)], lsem.at[0]),
             pltpu.make_async_copy(pos_ref, pos_all_ref.at[me], lsem.at[1])]
    for cp in local:
        cp.start()
    arrived(0, x_nbr, 0)
    start(6, region(x_nbr, 0), x_nbr, 0, y_nbr)
    start(8, region(x_nbr, 0), x_nbr, 0, c_nbr)
    arrived(3, y_nbr, 1)
    start(7, region(y_nbr, 1), y_nbr, 1, x_nbr)
    start(11, region(y_nbr, 1), y_nbr, 1, c_nbr)
    arrived(1, x_nbr, 1)
    start(9, region(x_nbr, 1), x_nbr, 1, c_nbr)
    arrived(2, y_nbr, 0)
    start(10, region(y_nbr, 0), y_nbr, 0, c_nbr)
    arrived(6, diag, 0)
    start(12, region(diag, 0), diag, 0, c_nbr)
    arrived(7, diag, 1)
    start(13, region(diag, 1), diag, 1, c_nbr)
    arrived(4, c_nbr, 0)
    arrived(5, c_nbr, 1)
    arrived(8, x_nbr + d_c, 0)
    arrived(9, x_nbr + d_c, 1)
    arrived(10, y_nbr + d_c, 0)
    arrived(11, y_nbr + d_c, 1)
    arrived(12, diag + d_c, 0)
    arrived(13, diag + d_c, 1)
    for cp in list(sends.values()) + pos_copies:
        cp.wait_send()
    for r in range(1, 8):
        src = lax.rem(me + 8 - r, 8)
        pltpu.make_async_remote_copy(src_ref=pos_all_ref.at[src], dst_ref=pos_all_ref.at[src], send_sem=psend.at[r - 1],
                                     recv_sem=precv.at[r - 1], device_id={'sp': me}, device_id_type=pl.DeviceIdType.MESH).wait_recv()
    for cp in local:
        cp.wait()


def gather_tokens(normed, positions):
    rows, feat = normed.shape
    pos_pad = jnp.pad(positions, (0, 1024 - rows)).reshape(8, 128)
    h_all, pos_all = pl.pallas_call(
        gather_kernel, name='gather_tokens',
        in_specs=[pl.BlockSpec(memory_space=pltpu.VMEM)] * 2, out_specs=[pl.BlockSpec(memory_space=pl.ANY)] * 2,
        out_shape=[jax.ShapeDtypeStruct((8 * rows, feat), BF16), jax.ShapeDtypeStruct((8, 8, 128), jnp.int32)],
        scratch_shapes=[pltpu.SemaphoreType.DMA((14,)), pltpu.SemaphoreType.DMA((14,)), pltpu.SemaphoreType.DMA((7,)),
                        pltpu.SemaphoreType.DMA((7,)), pltpu.SemaphoreType.DMA((2,))],
        compiler_params=pltpu.CompilerParams(collective_id=3, has_side_effects=True, vmem_limit_bytes=VLIM),
        cost_estimate=pl.CostEstimate(flops=0, bytes_accessed=16 * rows * feat, transcendentals=0),
    )(normed, pos_pad)
    return h_all, pos_all.reshape(8, 1024)[:, :rows].reshape(-1)


def rope_tables(positions):
    lane = jnp.arange(HEAD_DIM)
    inv_freq = ROPE_BASE ** (-(lane - lane % 2).astype(F32) / HEAD_DIM)
    angles = positions.astype(F32)[:, None] * inv_freq[None, :]
    sign = jnp.where(lane % 2 == 0, -1.0, 1.0).astype(F32)
    return jnp.cos(angles), jnp.sin(angles) * sign[None, :]


def swap_pairs(val):
    lane = lax.broadcasted_iota(jnp.int32, val.shape, 1)
    return jnp.where(lane % 2 == 0, pltpu.roll(val, HEAD_DIM - 1, 1), pltpu.roll(val, 1, 1))


def rotate(val, cos_t, sin_t):
    return val * cos_t + swap_pairs(val) * sin_t


def dot_f32(lhs, rhs):
    return jnp.dot(lhs, rhs, preferred_element_type=F32)


def proj_kernel(heads, h_ref, w_ref, cos_ref, sin_ref, q_ref, k_ref, v_ref, qt_ref, kt_ref, vt_ref):
    cos_t, sin_t = cos_ref[...], sin_ref[...]
    width = heads * HEAD_DIM
    for idx, (out, out_t) in enumerate(((q_ref, qt_ref), (k_ref, kt_ref), (v_ref, vt_ref))):
        prod = dot_f32(h_ref[...], w_ref[:, idx * width:(idx + 1) * width])
        for n in range(heads):
            val = prod[:, n * HEAD_DIM:(n + 1) * HEAD_DIM]
            if idx < 2:
                val = rotate(val, cos_t, sin_t)
            val = val.astype(BF16)
            out[n] = val
            out_t[n] = val.T


def project(h_all, w_cat, cos_t, sin_t, heads):
    rows, feat = h_all.shape
    width = w_cat.shape[1]
    bm = math.gcd(rows, 512)
    tok = pl.BlockSpec((heads, bm, HEAD_DIM), lambda i: (0, i, 0))
    tr = pl.BlockSpec((heads, HEAD_DIM, bm), lambda i: (0, 0, i))
    tab = pl.BlockSpec((bm, HEAD_DIM), lambda i: (i, 0))
    s_tok = jax.ShapeDtypeStruct((heads, rows, HEAD_DIM), BF16)
    s_tr = jax.ShapeDtypeStruct((heads, HEAD_DIM, rows), BF16)
    return pl.pallas_call(
        functools.partial(proj_kernel, heads), grid=(rows // bm,), name='qkv_proj',
        in_specs=[pl.BlockSpec((bm, feat), lambda i: (i, 0)), pl.BlockSpec((feat, width), lambda i: (0, 0)), tab, tab],
        out_specs=[tok] * 3 + [tr] * 3, out_shape=[s_tok] * 3 + [s_tr] * 3,
        compiler_params=pltpu.CompilerParams(vmem_limit_bytes=VLIM),
        cost_estimate=pl.CostEstimate(flops=2 * rows * feat * width, bytes_accessed=2 * rows * feat, transcendentals=0),
    )(h_all, w_cat, cos_t, sin_t)


def fwd_kernel(blk, heads, k_ref, qt_ref, vt_ref, o_ref, ot_ref, lse_ref, acc_ref):
    qi = pl.program_id(0)
    acc_ref[...] = jnp.zeros_like(acc_ref)

    def chunk(j, carry, masked):
        start = pl.multiple_of(j * blk, blk)
        scores = [dot_f32(k_ref[n, pl.ds(start, blk), :], qt_ref[n]) for n in range(heads)]
        if masked:
            key = lax.broadcasted_iota(jnp.int32, (blk, blk), 0)
            qry = lax.broadcasted_iota(jnp.int32, (blk, blk), 1)
            scores = [jnp.where(key <= qry, s_t, NEG) for s_t in scores]
        out = []
        for n in range(heads):
            m_old, l_old = carry[n]
            s_t = scores[n]
            m_new = jnp.maximum(m_old, jnp.max(s_t, axis=0, keepdims=True) * C2)
            p_t = jnp.exp2(s_t * C2 - m_new)
            alpha = jnp.exp2(m_old - m_new)
            l_new = l_old * alpha + jnp.sum(p_t, axis=0, keepdims=True)
            acc_ref[n] = acc_ref[n] * alpha + dot_f32(vt_ref[n, :, pl.ds(start, blk)], p_t.astype(BF16))
            out.append((m_new, l_new))
        return tuple(out)

    init = tuple((jnp.full((1, blk), NEG, F32), jnp.zeros((1, blk), F32)) for _ in range(heads))
    carry = lax.fori_loop(0, qi, lambda j, c: chunk(j, c, False), init)
    carry = chunk(qi, carry, True)
    for n in range(heads):
        m_fin, l_fin = carry[n]
        o_t = acc_ref[n] / l_fin
        ot_ref[n] = o_t
        o_ref[:, n * HEAD_DIM:(n + 1) * HEAD_DIM] = o_t.T.astype(BF16)
        lse_ref[n] = m_fin + jnp.log2(l_fin)


def attn_fwd(k, q_t, v_t):
    heads, rows, _ = k.shape
    blk = math.gcd(rows, 768)
    full = pl.BlockSpec((heads, rows, HEAD_DIM), lambda i: (0, 0, 0))
    full_t = pl.BlockSpec((heads, HEAD_DIM, rows), lambda i: (0, 0, 0))
    blk_t = pl.BlockSpec((heads, HEAD_DIM, blk), lambda i: (0, 0, i))
    return pl.pallas_call(
        functools.partial(fwd_kernel, blk, heads), grid=(rows // blk,), name='attn_fwd',
        in_specs=[full, blk_t, full_t],
        out_specs=[pl.BlockSpec((blk, heads * HEAD_DIM), lambda i: (i, 0)), blk_t,
                   pl.BlockSpec((heads, 1, blk), lambda i: (0, 0, i))],
        out_shape=[jax.ShapeDtypeStruct((rows, heads * HEAD_DIM), BF16),
                   jax.ShapeDtypeStruct((heads, HEAD_DIM, rows), F32),
                   jax.ShapeDtypeStruct((heads, 1, rows), F32)],
        scratch_shapes=[pltpu.VMEM((heads, HEAD_DIM, blk), F32)],
        compiler_params=pltpu.CompilerParams(vmem_limit_bytes=VLIM),
        cost_estimate=pl.CostEstimate(flops=4 * heads * rows * rows * HEAD_DIM, bytes_accessed=8 * heads * rows * HEAD_DIM,
                                      transcendentals=heads * rows * rows // 2),
    )(k, q_t, v_t)


def do_kernel(heads, g_ref, wo_ref, ot_ref, do_ref, dot_ref, dsum_ref, dwo_ref, acc_ref):
    step = pl.program_id(0)

    @pl.when(step == 0)
    def _():
        acc_ref[...] = jnp.zeros_like(acc_ref)

    prod = dot_f32(g_ref[...], wo_ref[...])
    for n in range(heads):
        own = slice(n * HEAD_DIM, (n + 1) * HEAD_DIM)
        val = prod[:, own].astype(BF16)
        val_t = val.T
        o_t = ot_ref[n]
        do_ref[n] = val
        dot_ref[n] = val_t
        dsum_ref[n] = jnp.sum(val_t.astype(F32) * o_t, axis=0, keepdims=True)
        acc_ref[own, :] += dot_f32(o_t.astype(BF16), g_ref[...])

    @pl.when(step == pl.num_programs(0) - 1)
    def _():
        dwo_ref[...] = acc_ref[...].astype(BF16)


def project_do(g_all, wo_cols, o_t, heads):
    rows, feat = g_all.shape
    width = wo_cols.shape[1]
    bm = math.gcd(rows, 1024)
    tok = pl.BlockSpec((heads, bm, HEAD_DIM), lambda i: (0, i, 0))
    tr = pl.BlockSpec((heads, HEAD_DIM, bm), lambda i: (0, 0, i))
    return pl.pallas_call(
        functools.partial(do_kernel, heads), grid=(rows // bm,), name='do_dwo',
        in_specs=[pl.BlockSpec((bm, feat), lambda i: (i, 0)), pl.BlockSpec((feat, width), lambda i: (0, 0)), tr],
        out_specs=[tok, tr, pl.BlockSpec((heads, 1, bm), lambda i: (0, 0, i)), pl.BlockSpec((width, feat), lambda i: (0, 0))],
        out_shape=[jax.ShapeDtypeStruct((heads, rows, HEAD_DIM), BF16), jax.ShapeDtypeStruct((heads, HEAD_DIM, rows), BF16),
                   jax.ShapeDtypeStruct((heads, 1, rows), F32), jax.ShapeDtypeStruct((width, feat), BF16)],
        scratch_shapes=[pltpu.VMEM((width, feat), F32)],
        compiler_params=pltpu.CompilerParams(vmem_limit_bytes=VLIM),
        cost_estimate=pl.CostEstimate(flops=4 * rows * feat * width, bytes_accessed=2 * rows * feat, transcendentals=0),
    )(g_all, wo_cols, o_t)


def bwd_kernel(blk, n_blk, k_ref, v_ref, kt_ref, q_ref, qt_ref, do_ref, dot_ref, lse_ref, dsum_ref, cos_ref, sin_ref,
               g_ref, dqt_ref, dk_ref, dv_ref):
    kj = pl.program_id(0)
    half = blk // 2

    @pl.when(kj == 0)
    def _():
        dqt_ref[...] = jnp.zeros_like(dqt_ref)

    def tile(k_lo, k_num, q_start, q_num, masked, first):
        keys = slice(k_lo, k_lo + k_num)
        cols = pl.ds(q_start, q_num)
        p_t = jnp.exp2(dot_f32(k_ref[0, keys, :], qt_ref[0, :, cols]) * C2 - lse_ref[0, :, cols])
        if masked:
            key = lax.broadcasted_iota(jnp.int32, p_t.shape, 0)
            qry = lax.broadcasted_iota(jnp.int32, p_t.shape, 1)
            p_t = jnp.where(key <= qry, p_t, 0.0)
        dp_t = dot_f32(v_ref[0, keys, :], dot_ref[0, :, cols])
        ds_t = (p_t * ((dp_t - dsum_ref[0, :, cols]) * SCALE)).astype(BF16)
        dv_new = dot_f32(p_t.astype(BF16), do_ref[0, cols, :])
        dk_new = dot_f32(ds_t, q_ref[0, cols, :])
        if first:
            dv_ref[keys, :] = dv_new
            dk_ref[keys, :] = dk_new
        else:
            dv_ref[keys, :] += dv_new
            dk_ref[keys, :] += dk_new
        dqt_ref[:, cols] += dot_f32(kt_ref[0, :, keys], ds_t)

    base = pl.multiple_of(kj * blk, blk)
    tile(0, half, base, half, True, True)
    tile(half, half, base + half, half, True, True)
    tile(0, half, base + half, half, False, False)

    def body(i, carry):
        tile(0, blk, pl.multiple_of(i * blk, blk), blk, False, False)
        return carry

    lax.fori_loop(kj + 1, n_blk, body, 0)
    cos_t, sin_t = cos_ref[...], -sin_ref[...]
    d_q = dqt_ref[:, pl.ds(base, blk)].T.astype(BF16).astype(F32)
    g_ref[:, :HEAD_DIM] = rotate(d_q, cos_t, sin_t).astype(BF16)
    g_ref[:, HEAD_DIM:2 * HEAD_DIM] = rotate(dk_ref[...].astype(BF16).astype(F32), cos_t, sin_t).astype(BF16)
    g_ref[:, 2 * HEAD_DIM:] = dv_ref[...].astype(BF16)


def attn_bwd(n, k, v, k_t, q, q_t, d_o, d_ot, lse, dsum, cos_t, sin_t):
    _, rows, _ = k.shape
    blk = math.gcd(rows, 1024)
    n_blk = rows // blk
    blk_tok = pl.BlockSpec((1, blk, HEAD_DIM), lambda j: (n, j, 0))
    blk_tr = pl.BlockSpec((1, HEAD_DIM, blk), lambda j: (n, 0, j))
    full = pl.BlockSpec((1, rows, HEAD_DIM), lambda j: (n, 0, 0))
    full_t = pl.BlockSpec((1, HEAD_DIM, rows), lambda j: (n, 0, 0))
    vec = pl.BlockSpec((1, 1, rows), lambda j: (n, 0, 0))
    tab = pl.BlockSpec((blk, HEAD_DIM), lambda j: (j, 0))
    return pl.pallas_call(
        functools.partial(bwd_kernel, blk, n_blk), grid=(n_blk,), name='attn_bwd',
        in_specs=[blk_tok, blk_tok, blk_tr, full, full_t, full, full_t, vec, vec, tab, tab],
        out_specs=pl.BlockSpec((blk, 3 * HEAD_DIM), lambda j: (j, 0)),
        out_shape=jax.ShapeDtypeStruct((rows, 3 * HEAD_DIM), BF16),
        scratch_shapes=[pltpu.VMEM((HEAD_DIM, rows), F32), pltpu.VMEM((blk, HEAD_DIM), F32), pltpu.VMEM((blk, HEAD_DIM), F32)],
        compiler_params=pltpu.CompilerParams(vmem_limit_bytes=VLIM),
        cost_estimate=pl.CostEstimate(flops=10 * rows * rows * HEAD_DIM, bytes_accessed=20 * rows * HEAD_DIM,
                                      transcendentals=rows * rows // 2),
    )(k, v, k_t, q, q_t, d_o, d_ot, lse, dsum, cos_t, sin_t)


def dw_kernel(h_ref, g_ref, out_ref, acc_ref):
    step = pl.program_id(0)
    feat = h_ref.shape[1]
    tile = math.gcd(feat, 512)

    @pl.when(step == 0)
    def _():
        acc_ref[...] = jnp.zeros_like(acc_ref)

    def body(i, carry):
        cols = pl.ds(pl.multiple_of(i * tile, tile), tile)
        acc_ref[:, cols] += lax.dot_general(g_ref[...], h_ref[:, cols], (((0,), (0,)), ((), ())), preferred_element_type=F32)
        return carry

    lax.fori_loop(0, feat // tile, body, 0)

    @pl.when(step == pl.num_programs(0) - 1)
    def _():
        def flip(i, carry):
            rows = pl.ds(pl.multiple_of(i * tile, tile), tile)
            out_ref[rows, :] = acc_ref[:, rows].astype(BF16).T
            return carry

        lax.fori_loop(0, feat // tile, flip, 0)


def weight_grad(h_all, g_tok):
    rows, feat = h_all.shape
    width = g_tok.shape[1]
    bm = math.gcd(rows, 1024)
    return pl.pallas_call(
        dw_kernel, grid=(rows // bm,), name='weight_grad',
        in_specs=[pl.BlockSpec((bm, feat), lambda i: (i, 0)), pl.BlockSpec((bm, width), lambda i: (i, 0))],
        out_specs=pl.BlockSpec((feat, width), lambda i: (0, 0)), out_shape=jax.ShapeDtypeStruct((feat, width), BF16),
        scratch_shapes=[pltpu.VMEM((width, feat), F32)],
        compiler_params=pltpu.CompilerParams(vmem_limit_bytes=VLIM),
        cost_estimate=pl.CostEstimate(flops=2 * rows * feat * width, bytes_accessed=2 * rows * feat, transcendentals=0),
    )(h_all, g_tok)


def out_kernel(o_ref, w_ref, out_ref, acc_ref):
    step = pl.program_id(0)
    tile = math.gcd(w_ref.shape[1], 512)

    @pl.when(step == 0)
    def _():
        acc_ref[...] = jnp.zeros_like(acc_ref)

    def body(i, carry):
        cols = pl.ds(pl.multiple_of(i * tile, tile), tile)
        acc_ref[:, cols] += dot_f32(o_ref[0], w_ref[:, cols])
        return carry

    lax.fori_loop(0, w_ref.shape[1] // tile, body, 0)

    @pl.when(step == pl.num_programs(0) - 1)
    def _():
        out_ref[...] = acc_ref[...].astype(BF16)


def out_proj(o_own, w_o):
    devs, rows, width = o_own.shape
    feat = w_o.shape[1]
    return pl.pallas_call(
        out_kernel, grid=(devs,), name='out_proj',
        in_specs=[pl.BlockSpec((1, rows, width), lambda j: (j, 0, 0)), pl.BlockSpec((width, feat), lambda j: (j, 0))],
        out_specs=pl.BlockSpec((rows, feat), lambda j: (0, 0)), out_shape=jax.ShapeDtypeStruct((rows, feat), BF16),
        scratch_shapes=[pltpu.VMEM((rows, feat), F32)],
        compiler_params=pltpu.CompilerParams(vmem_limit_bytes=VLIM),
        cost_estimate=pl.CostEstimate(flops=2 * devs * rows * feat * width, bytes_accessed=2 * devs * feat * width, transcendentals=0),
    )(o_own, w_o)


def dh_kernel(heads, *refs):
    g_refs, w_refs = refs[:heads], refs[heads:heads + 3]
    x_ref, lnw_ref, dx_ref, dlnw_ref, acc_ref = refs[heads + 3:]
    step = pl.program_id(0)
    rows, feat = acc_ref.shape
    tile = math.gcd(feat, 512)

    @pl.when(step == 0)
    def _():
        acc_ref[...] = jnp.zeros_like(acc_ref)
        dlnw_ref[...] = jnp.zeros_like(dlnw_ref)

    def body(i, carry):
        cols = pl.ds(pl.multiple_of(i * tile, tile), tile)
        total = acc_ref[:, cols]
        for idx in range(3):
            lanes = slice(idx * HEAD_DIM, (idx + 1) * HEAD_DIM)
            lhs = jnp.concatenate([g_ref[0, :, lanes] for g_ref in g_refs], axis=1)
            total += lax.dot_general(lhs, w_refs[idx][cols, :], (((1,), (1,)), ((), ())), preferred_element_type=F32)
        acc_ref[:, cols] = total
        return carry

    lax.fori_loop(0, feat // tile, body, 0)

    @pl.when(step == pl.num_programs(0) - 1)
    def _():
        bm = math.gcd(rows, 64)
        weight = lnw_ref[...].astype(F32)

        def norm_bwd(i, carry):
            own = pl.ds(pl.multiple_of(i * bm, bm), bm)
            hid = x_ref[own, :].astype(F32)
            d_h = acc_ref[own, :]
            centered = hid - jnp.mean(hid, axis=-1, keepdims=True)
            rstd = lax.rsqrt(jnp.mean(centered * centered, axis=-1, keepdims=True) + LN_EPS)
            x_hat = centered * rstd
            dlnw_ref[...] += jnp.sum(d_h * x_hat, axis=0, keepdims=True)
            d_hat = d_h * weight
            mean_d = jnp.mean(d_hat, axis=-1, keepdims=True)
            mean_dx = jnp.mean(d_hat * x_hat, axis=-1, keepdims=True)
            dx_ref[own, :] = (rstd * (d_hat - mean_d - x_hat * mean_dx)).astype(BF16)
            return carry

        lax.fori_loop(0, rows // bm, norm_bwd, 0)


def hidden_grad(g_owns, weights, hidden, ln_weight):
    devs, rows, width = g_owns[0].shape
    heads = len(g_owns)
    feat = hidden.shape[1]
    whole = pl.BlockSpec((rows, feat), lambda j: (0, 0))
    vec = pl.BlockSpec((1, feat), lambda j: (0, 0))
    return pl.pallas_call(
        functools.partial(dh_kernel, heads), grid=(devs,), name='hidden_grad',
        in_specs=[pl.BlockSpec((1, rows, width), lambda j: (j, 0, 0))] * heads
        + [pl.BlockSpec((feat, heads * HEAD_DIM), lambda j: (0, j))] * 3 + [whole, vec],
        out_specs=[whole, vec],
        out_shape=[jax.ShapeDtypeStruct((rows, feat), BF16), jax.ShapeDtypeStruct((1, feat), F32)],
        scratch_shapes=[pltpu.VMEM((rows, feat), F32)],
        compiler_params=pltpu.CompilerParams(vmem_limit_bytes=VLIM),
        cost_estimate=pl.CostEstimate(flops=2 * devs * heads * rows * feat * width, bytes_accessed=6 * feat * feat,
                                      transcendentals=rows),
    )(*g_owns, *weights, hidden, ln_weight[None, :])


def copy_kernel(a_ref, out_ref):
    out_ref[...] = a_ref[...]


def copy_rows(val):
    rows, feat = val.shape
    spec = pl.BlockSpec((math.gcd(rows, 256), feat), lambda i: (i, 0))
    return pl.pallas_call(
        copy_kernel, grid=(rows // spec.block_shape[0],), name='copy_rows', in_specs=[spec], out_specs=spec,
        out_shape=jax.ShapeDtypeStruct(val.shape, val.dtype),
        cost_estimate=pl.CostEstimate(flops=rows * feat, bytes_accessed=4 * rows * feat, transcendentals=0),
    )(val)


def place_kernel(a_ref, *refs):
    for idx, out in enumerate(refs[-3:]):
        out[...] = a_ref[0, :, idx * HEAD_DIM:(idx + 1) * HEAD_DIM]


def place_slot(n, heads, gathered, grads):
    devs, feat, width = gathered.shape
    spec = pl.BlockSpec((feat, HEAD_DIM), lambda j: (0, j * heads + n))
    shape = jax.ShapeDtypeStruct((feat, devs * heads * HEAD_DIM), BF16)
    return pl.pallas_call(
        place_kernel, grid=(devs,), name='place',
        in_specs=[pl.BlockSpec((1, feat, width), lambda j: (j, 0, 0))] + [pl.BlockSpec(memory_space=pl.ANY)] * len(grads),
        out_specs=[spec] * 3, out_shape=[shape] * 3,
        input_output_aliases={1 + i: i for i in range(len(grads))},
        compiler_params=pltpu.CompilerParams(vmem_limit_bytes=VLIM),
        cost_estimate=pl.CostEstimate(flops=devs * feat * width, bytes_accessed=4 * devs * feat * width, transcendentals=0),
    )(gathered, *grads)


def solution(mesh):
    sp_size = mesh.shape['sp']
    row_spec = P(('dp', 'sp'), None)
    pos_spec = P(('dp', 'sp'))
    full_spec = P(None, None)
    grad_spec = P('dp', None)

    def layer_step(hidden, positions, d_attn, ln_weight, w_q, w_k, w_v, w_o):
        _, all_width = w_q.shape
        width = all_width // sp_size
        heads = width // HEAD_DIM
        me = lax.axis_index('sp')
        normed = layer_norm(hidden, ln_weight)
        h_all, pos_all = gather_tokens(normed, positions)
        cos_t, sin_t = rope_tables(pos_all)
        own = lambda w: lax.dynamic_slice_in_dim(w, me * width, width, 1)
        w_cat = jnp.concatenate([own(w_q), own(w_k), own(w_v)], axis=1)
        wo_cols = lax.dynamic_slice_in_dim(w_o, me * width, width, 0).T
        g_dep, h_all = lax.optimization_barrier((d_attn, h_all))
        g_all = lax.all_gather(g_dep, 'sp', axis=0, tiled=True)
        q, k, v, q_t, k_t, v_t = project(h_all, w_cat, cos_t, sin_t, heads)
        o_tok, o_t, lse = attn_fwd(k, q_t, v_t)

        row_major = Layout(major_to_minor=(0, 1, 2))

        def to_owner(val):
            val = with_layout_constraint(val.reshape(sp_size, -1, val.shape[1]), row_major)
            val = with_layout_constraint(lax.all_to_all(val, 'sp', 0, 0, tiled=True), row_major)
            return val

        o_tok, g_all = lax.optimization_barrier((o_tok, g_all))
        o_own = to_owner(o_tok)
        d_o, d_ot, dsum, dw_o = project_do(g_all, wo_cols, o_t, heads)
        dw_o = lax.all_gather(dw_o, 'sp', axis=0, tiled=True)
        dw_o = copy_rows(dw_o)
        attn_out = out_proj(o_own, w_o)
        d_ws = []
        g_owns = []
        for n in range(heads):
            g_tok = attn_bwd(n, k, v, k_t, q, q_t, d_o, d_ot, lse, dsum, cos_t, sin_t)
            g_owns.append(to_owner(g_tok))
            d_w = weight_grad(h_all, g_tok)
            d_ws.append(lax.all_gather(d_w, 'sp', axis=0))
        grads = ()
        for n in range(heads):
            grads = place_slot(n, heads, d_ws[n], grads)
        d_hid, d_lnw = hidden_grad(g_owns, (w_q, w_k, w_v), hidden, ln_weight)
        d_lnw = lax.psum(d_lnw[0], 'sp')
        return (attn_out, d_hid, d_lnw.astype(BF16), grads[0], grads[1], grads[2], dw_o)

    return jax.shard_map(layer_step, mesh=mesh,
                         in_specs=(row_spec, pos_spec, row_spec, P(None), full_spec, full_spec, full_spec, full_spec),
                         out_specs=(row_spec, row_spec, P('dp'), grad_spec, grad_spec, grad_spec, grad_spec),
                         check_vma=False)
```

```python
import functools
import math
import jax
import jax.numpy as jnp
from jax import lax
from jax.experimental import pallas as pl
from jax.experimental.layout import Layout, with_layout_constraint
from jax.experimental.pallas import tpu as pltpu
from jax.sharding import PartitionSpec as P

HEAD_DIM = 128
LN_EPS = 1e-5
ROPE_BASE = 10000.0
SCALE = HEAD_DIM ** -0.5
LOG2E = math.log2(math.e)
C2 = SCALE * LOG2E
NEG = -1e30
VLIM = 56 * 1024 * 1024
F32 = jnp.float32
BF16 = jnp.bfloat16


def norm_f32(hid_f32, weight_f32):
    mean_val = jnp.mean(hid_f32, axis=-1, keepdims=True)
    centered = hid_f32 - mean_val
    var_val = jnp.mean(centered * centered, axis=-1, keepdims=True)
    return centered * lax.rsqrt(var_val + LN_EPS) * weight_f32


def norm_kernel(x_ref, w_ref, out_ref):
    out_ref[...] = norm_f32(x_ref[...].astype(F32), w_ref[...].astype(F32)).astype(BF16)


def layer_norm(hidden, weight):
    rows, feat = hidden.shape
    bm = math.gcd(rows, 256)
    spec = pl.BlockSpec((bm, feat), lambda i: (i, 0))
    return pl.pallas_call(
        norm_kernel, grid=(rows // bm,), name='layer_norm',
        in_specs=[spec, pl.BlockSpec((1, feat), lambda i: (0, 0))], out_specs=spec,
        out_shape=jax.ShapeDtypeStruct((rows, feat), BF16),
        cost_estimate=pl.CostEstimate(flops=10 * rows * feat, bytes_accessed=4 * rows * feat, transcendentals=rows),
    )(hidden, weight[None, :])


def gather_kernel(h_ref, pos_ref, all_ref, pos_all_ref, send, recv, psend, precv, lsem):
    me = lax.axis_index('sp')
    rows = h_ref.shape[0]
    half = rows // 2
    core, x_pos, y_pos = lax.rem(me, 2), lax.rem(me // 2, 2), me // 4
    d_x, d_y, d_c = 2 - 4 * x_pos, 4 - 8 * y_pos, 1 - 2 * core
    x_nbr, y_nbr, c_nbr = me + d_x, me + d_y, me + d_c
    diag = me + d_x + d_y

    barrier = pltpu.get_barrier_semaphore()
    for r in range(1, 8):
        pl.semaphore_signal(barrier, inc=1, device_id={'sp': lax.rem(me + r, 8)}, device_id_type=pl.DeviceIdType.MESH)
    pl.semaphore_wait(barrier, 7)

    def region(owner, part):
        return all_ref.at[pl.ds(pl.multiple_of(owner * rows + part * half, half), half)]

    def copy(k, src, owner, part, dst):
        return pltpu.make_async_remote_copy(src_ref=src, dst_ref=region(owner, part), send_sem=send.at[k], recv_sem=recv.at[k],
                                            device_id={'sp': dst}, device_id_type=pl.DeviceIdType.MESH)

    def own(part):
        return h_ref.at[pl.ds(part * half, half)]

    pos_copies = []
    for r in range(1, 8):
        cp = pltpu.make_async_remote_copy(src_ref=pos_ref, dst_ref=pos_all_ref.at[me], send_sem=psend.at[r - 1], recv_sem=precv.at[r - 1],
                                          device_id={'sp': lax.rem(me + r, 8)}, device_id_type=pl.DeviceIdType.MESH)
        cp.start()
        pos_copies.append(cp)
    sends = {}

    def start(k, src, owner, part, dst):
        sends[k] = copy(k, src, owner, part, dst)
        sends[k].start()

    def arrived(k, owner, part):
        copy(k, region(owner, part), owner, part, me).wait_recv()

    start(0, own(0), me, 0, x_nbr)
    start(3, own(1), me, 1, y_nbr)
    start(1, own(1), me, 1, x_nbr)
    start(2, own(0), me, 0, y_nbr)
    start(4, own(0), me, 0, c_nbr)
    start(5, own(1), me, 1, c_nbr)
    local = [pltpu.make_async_copy(h_ref, all_ref.at[pl.ds(pl.multiple_of(me * rows, rows), rows)], lsem.at[0]),
             pltpu.make_async_copy(pos_ref, pos_all_ref.at[me], lsem.at[1])]
    for cp in local:
        cp.start()
    arrived(0, x_nbr, 0)
    start(6, region(x_nbr, 0), x_nbr, 0, y_nbr)
    start(8, region(x_nbr, 0), x_nbr, 0, c_nbr)
    arrived(3, y_nbr, 1)
    start(7, region(y_nbr, 1), y_nbr, 1, x_nbr)
    start(11, region(y_nbr, 1), y_nbr, 1, c_nbr)
    arrived(1, x_nbr, 1)
    start(9, region(x_nbr, 1), x_nbr, 1, c_nbr)
    arrived(2, y_nbr, 0)
    start(10, region(y_nbr, 0), y_nbr, 0, c_nbr)
    arrived(6, diag, 0)
    start(12, region(diag, 0), diag, 0, c_nbr)
    arrived(7, diag, 1)
    start(13, region(diag, 1), diag, 1, c_nbr)
    arrived(4, c_nbr, 0)
    arrived(5, c_nbr, 1)
    arrived(8, x_nbr + d_c, 0)
    arrived(9, x_nbr + d_c, 1)
    arrived(10, y_nbr + d_c, 0)
    arrived(11, y_nbr + d_c, 1)
    arrived(12, diag + d_c, 0)
    arrived(13, diag + d_c, 1)
    for cp in list(sends.values()) + pos_copies:
        cp.wait_send()
    for r in range(1, 8):
        src = lax.rem(me + 8 - r, 8)
        pltpu.make_async_remote_copy(src_ref=pos_all_ref.at[src], dst_ref=pos_all_ref.at[src], send_sem=psend.at[r - 1],
                                     recv_sem=precv.at[r - 1], device_id={'sp': me}, device_id_type=pl.DeviceIdType.MESH).wait_recv()
    for cp in local:
        cp.wait()


def gather_tokens(normed, positions):
    rows, feat = normed.shape
    pos_pad = jnp.pad(positions, (0, 1024 - rows)).reshape(8, 128)
    h_all, pos_all = pl.pallas_call(
        gather_kernel, name='gather_tokens',
        in_specs=[pl.BlockSpec(memory_space=pltpu.VMEM)] * 2, out_specs=[pl.BlockSpec(memory_space=pl.ANY)] * 2,
        out_shape=[jax.ShapeDtypeStruct((8 * rows, feat), BF16), jax.ShapeDtypeStruct((8, 8, 128), jnp.int32)],
        scratch_shapes=[pltpu.SemaphoreType.DMA((14,)), pltpu.SemaphoreType.DMA((14,)), pltpu.SemaphoreType.DMA((7,)),
                        pltpu.SemaphoreType.DMA((7,)), pltpu.SemaphoreType.DMA((2,))],
        compiler_params=pltpu.CompilerParams(collective_id=3, has_side_effects=True, vmem_limit_bytes=VLIM),
        cost_estimate=pl.CostEstimate(flops=0, bytes_accessed=16 * rows * feat, transcendentals=0),
    )(normed, pos_pad)
    return h_all, pos_all.reshape(8, 1024)[:, :rows].reshape(-1)


def rope_tables(positions):
    lane = jnp.arange(HEAD_DIM)
    inv_freq = ROPE_BASE ** (-(lane - lane % 2).astype(F32) / HEAD_DIM)
    angles = positions.astype(F32)[:, None] * inv_freq[None, :]
    sign = jnp.where(lane % 2 == 0, -1.0, 1.0).astype(F32)
    return jnp.cos(angles), jnp.sin(angles) * sign[None, :]


def swap_pairs(val):
    lane = lax.broadcasted_iota(jnp.int32, val.shape, 1)
    return jnp.where(lane % 2 == 0, pltpu.roll(val, HEAD_DIM - 1, 1), pltpu.roll(val, 1, 1))


def rotate(val, cos_t, sin_t):
    return val * cos_t + swap_pairs(val) * sin_t


def dot_f32(lhs, rhs):
    return jnp.dot(lhs, rhs, preferred_element_type=F32)


def proj_kernel(heads, me_ref, h_ref, wq_ref, wk_ref, wv_ref, cos_ref, sin_ref, q_ref, k_ref, v_ref, qt_ref, kt_ref, vt_ref):
    cos_t, sin_t = cos_ref[...], sin_ref[...]
    w_refs = (wq_ref, wk_ref, wv_ref)
    for idx, (out, out_t) in enumerate(((q_ref, qt_ref), (k_ref, kt_ref), (v_ref, vt_ref))):
        prod = dot_f32(h_ref[...], w_refs[idx][...])
        for n in range(heads):
            val = prod[:, n * HEAD_DIM:(n + 1) * HEAD_DIM]
            if idx < 2:
                val = rotate(val, cos_t, sin_t)
            val = val.astype(BF16)
            out[n] = val
            out_t[n] = val.T


def project(me, h_all, weights, cos_t, sin_t, heads):
    rows, feat = h_all.shape
    width = heads * HEAD_DIM
    bm = math.gcd(rows, 512)
    tok = pl.BlockSpec((heads, bm, HEAD_DIM), lambda i, m: (0, i, 0))
    tr = pl.BlockSpec((heads, HEAD_DIM, bm), lambda i, m: (0, 0, i))
    tab = pl.BlockSpec((bm, HEAD_DIM), lambda i, m: (i, 0))
    own = pl.BlockSpec((feat, width), lambda i, m: (0, m[0]))
    s_tok = jax.ShapeDtypeStruct((heads, rows, HEAD_DIM), BF16)
    s_tr = jax.ShapeDtypeStruct((heads, HEAD_DIM, rows), BF16)
    return pl.pallas_call(
        functools.partial(proj_kernel, heads), name='qkv_proj', out_shape=[s_tok] * 3 + [s_tr] * 3,
        grid_spec=pltpu.PrefetchScalarGridSpec(
            num_scalar_prefetch=1, grid=(rows // bm,),
            in_specs=[pl.BlockSpec((bm, feat), lambda i, m: (i, 0)), own, own, own, tab, tab],
            out_specs=[tok] * 3 + [tr] * 3),
        compiler_params=pltpu.CompilerParams(vmem_limit_bytes=VLIM),
        cost_estimate=pl.CostEstimate(flops=6 * rows * feat * width, bytes_accessed=2 * rows * feat, transcendentals=0),
    )(me[None], h_all, *weights, cos_t, sin_t)


def fwd_kernel(blk, heads, k_ref, qt_ref, vt_ref, o_ref, ot_ref, lse_ref, acc_ref):
    qi = pl.program_id(0)
    acc_ref[...] = jnp.zeros_like(acc_ref)

    def chunk(j, carry, masked):
        start = pl.multiple_of(j * blk, blk)
        scores = [dot_f32(k_ref[n, pl.ds(start, blk), :], qt_ref[n]) for n in range(heads)]
        if masked:
            key = lax.broadcasted_iota(jnp.int32, (blk, blk), 0)
            qry = lax.broadcasted_iota(jnp.int32, (blk, blk), 1)
            scores = [jnp.where(key <= qry, s_t, NEG) for s_t in scores]
        out = []
        for n in range(heads):
            m_old, l_old = carry[n]
            s_t = scores[n]
            m_new = jnp.maximum(m_old, jnp.max(s_t, axis=0, keepdims=True) * C2)
            p_t = jnp.exp2(s_t * C2 - m_new)
            alpha = jnp.exp2(m_old - m_new)
            l_new = l_old * alpha + jnp.sum(p_t, axis=0, keepdims=True)
            acc_ref[n] = acc_ref[n] * alpha + dot_f32(vt_ref[n, :, pl.ds(start, blk)], p_t.astype(BF16))
            out.append((m_new, l_new))
        return tuple(out)

    init = tuple((jnp.full((1, blk), NEG, F32), jnp.zeros((1, blk), F32)) for _ in range(heads))
    carry = lax.fori_loop(0, qi, lambda j, c: chunk(j, c, False), init)
    carry = chunk(qi, carry, True)
    for n in range(heads):
        m_fin, l_fin = carry[n]
        o_t = acc_ref[n] / l_fin
        ot_ref[n] = o_t
        o_ref[:, n * HEAD_DIM:(n + 1) * HEAD_DIM] = o_t.T.astype(BF16)
        lse_ref[n] = m_fin + jnp.log2(l_fin)


def attn_fwd(k, q_t, v_t):
    heads, rows, _ = k.shape
    blk = math.gcd(rows, 768)
    full = pl.BlockSpec((heads, rows, HEAD_DIM), lambda i: (0, 0, 0))
    full_t = pl.BlockSpec((heads, HEAD_DIM, rows), lambda i: (0, 0, 0))
    blk_t = pl.BlockSpec((heads, HEAD_DIM, blk), lambda i: (0, 0, i))
    return pl.pallas_call(
        functools.partial(fwd_kernel, blk, heads), grid=(rows // blk,), name='attn_fwd',
        in_specs=[full, blk_t, full_t],
        out_specs=[pl.BlockSpec((blk, heads * HEAD_DIM), lambda i: (i, 0)), blk_t,
                   pl.BlockSpec((heads, 1, blk), lambda i: (0, 0, i))],
        out_shape=[jax.ShapeDtypeStruct((rows, heads * HEAD_DIM), BF16),
                   jax.ShapeDtypeStruct((heads, HEAD_DIM, rows), F32),
                   jax.ShapeDtypeStruct((heads, 1, rows), F32)],
        scratch_shapes=[pltpu.VMEM((heads, HEAD_DIM, blk), F32)],
        compiler_params=pltpu.CompilerParams(vmem_limit_bytes=VLIM),
        cost_estimate=pl.CostEstimate(flops=4 * heads * rows * rows * HEAD_DIM, bytes_accessed=8 * heads * rows * HEAD_DIM,
                                      transcendentals=heads * rows * rows // 2),
    )(k, q_t, v_t)


def do_kernel(heads, g_ref, wo_ref, ot_ref, do_ref, dot_ref, dsum_ref, dwo_ref, acc_ref):
    step = pl.program_id(0)

    @pl.when(step == 0)
    def _():
        acc_ref[...] = jnp.zeros_like(acc_ref)

    prod = dot_f32(g_ref[...], wo_ref[...])
    for n in range(heads):
        own = slice(n * HEAD_DIM, (n + 1) * HEAD_DIM)
        val = prod[:, own].astype(BF16)
        val_t = val.T
        o_t = ot_ref[n]
        do_ref[n] = val
        dot_ref[n] = val_t
        dsum_ref[n] = jnp.sum(val_t.astype(F32) * o_t, axis=0, keepdims=True)
        acc_ref[own, :] += dot_f32(o_t.astype(BF16), g_ref[...])

    @pl.when(step == pl.num_programs(0) - 1)
    def _():
        dwo_ref[...] = acc_ref[...].astype(BF16)


def project_do(g_all, wo_cols, o_t, heads):
    rows, feat = g_all.shape
    width = wo_cols.shape[1]
    bm = math.gcd(rows, 1024)
    tok = pl.BlockSpec((heads, bm, HEAD_DIM), lambda i: (0, i, 0))
    tr = pl.BlockSpec((heads, HEAD_DIM, bm), lambda i: (0, 0, i))
    return pl.pallas_call(
        functools.partial(do_kernel, heads), grid=(rows // bm,), name='do_dwo',
        in_specs=[pl.BlockSpec((bm, feat), lambda i: (i, 0)), pl.BlockSpec((feat, width), lambda i: (0, 0)), tr],
        out_specs=[tok, tr, pl.BlockSpec((heads, 1, bm), lambda i: (0, 0, i)), pl.BlockSpec((width, feat), lambda i: (0, 0))],
        out_shape=[jax.ShapeDtypeStruct((heads, rows, HEAD_DIM), BF16), jax.ShapeDtypeStruct((heads, HEAD_DIM, rows), BF16),
                   jax.ShapeDtypeStruct((heads, 1, rows), F32), jax.ShapeDtypeStruct((width, feat), BF16)],
        scratch_shapes=[pltpu.VMEM((width, feat), F32)],
        compiler_params=pltpu.CompilerParams(vmem_limit_bytes=VLIM),
        cost_estimate=pl.CostEstimate(flops=4 * rows * feat * width, bytes_accessed=2 * rows * feat, transcendentals=0),
    )(g_all, wo_cols, o_t)


def bwd_kernel(blk, n_blk, k_ref, v_ref, kt_ref, q_ref, qt_ref, do_ref, dot_ref, lse_ref, dsum_ref, cos_ref, sin_ref,
               g_ref, dqt_ref, dk_ref, dv_ref):
    kj = pl.program_id(0)
    half = blk // 2

    @pl.when(kj == 0)
    def _():
        dqt_ref[...] = jnp.zeros_like(dqt_ref)

    def tile(k_lo, k_num, q_start, q_num, masked, first):
        keys = slice(k_lo, k_lo + k_num)
        cols = pl.ds(q_start, q_num)
        p_t = jnp.exp2(dot_f32(k_ref[0, keys, :], qt_ref[0, :, cols]) * C2 - lse_ref[0, :, cols])
        if masked:
            key = lax.broadcasted_iota(jnp.int32, p_t.shape, 0)
            qry = lax.broadcasted_iota(jnp.int32, p_t.shape, 1)
            p_t = jnp.where(key <= qry, p_t, 0.0)
        dp_t = dot_f32(v_ref[0, keys, :], dot_ref[0, :, cols])
        ds_t = (p_t * ((dp_t - dsum_ref[0, :, cols]) * SCALE)).astype(BF16)
        dv_new = dot_f32(p_t.astype(BF16), do_ref[0, cols, :])
        dk_new = dot_f32(ds_t, q_ref[0, cols, :])
        if first:
            dv_ref[keys, :] = dv_new
            dk_ref[keys, :] = dk_new
        else:
            dv_ref[keys, :] += dv_new
            dk_ref[keys, :] += dk_new
        dqt_ref[:, cols] += dot_f32(kt_ref[0, :, keys], ds_t)

    base = pl.multiple_of(kj * blk, blk)
    tile(0, half, base, half, True, True)
    tile(half, half, base + half, half, True, True)
    tile(0, half, base + half, half, False, False)

    def body(i, carry):
        tile(0, blk, pl.multiple_of(i * blk, blk), blk, False, False)
        return carry

    lax.fori_loop(kj + 1, n_blk, body, 0)
    cos_t, sin_t = cos_ref[...], -sin_ref[...]
    d_q = dqt_ref[:, pl.ds(base, blk)].T.astype(BF16).astype(F32)
    g_ref[:, :HEAD_DIM] = rotate(d_q, cos_t, sin_t).astype(BF16)
    g_ref[:, HEAD_DIM:2 * HEAD_DIM] = rotate(dk_ref[...].astype(BF16).astype(F32), cos_t, sin_t).astype(BF16)
    g_ref[:, 2 * HEAD_DIM:] = dv_ref[...].astype(BF16)


def attn_bwd(n, k, v, k_t, q, q_t, d_o, d_ot, lse, dsum, cos_t, sin_t):
    _, rows, _ = k.shape
    blk = math.gcd(rows, 1024)
    n_blk = rows // blk
    blk_tok = pl.BlockSpec((1, blk, HEAD_DIM), lambda j: (n, j, 0))
    blk_tr = pl.BlockSpec((1, HEAD_DIM, blk), lambda j: (n, 0, j))
    full = pl.BlockSpec((1, rows, HEAD_DIM), lambda j: (n, 0, 0))
    full_t = pl.BlockSpec((1, HEAD_DIM, rows), lambda j: (n, 0, 0))
    vec = pl.BlockSpec((1, 1, rows), lambda j: (n, 0, 0))
    tab = pl.BlockSpec((blk, HEAD_DIM), lambda j: (j, 0))
    return pl.pallas_call(
        functools.partial(bwd_kernel, blk, n_blk), grid=(n_blk,), name='attn_bwd',
        in_specs=[blk_tok, blk_tok, blk_tr, full, full_t, full, full_t, vec, vec, tab, tab],
        out_specs=pl.BlockSpec((blk, 3 * HEAD_DIM), lambda j: (j, 0)),
        out_shape=jax.ShapeDtypeStruct((rows, 3 * HEAD_DIM), BF16),
        scratch_shapes=[pltpu.VMEM((HEAD_DIM, rows), F32), pltpu.VMEM((blk, HEAD_DIM), F32), pltpu.VMEM((blk, HEAD_DIM), F32)],
        compiler_params=pltpu.CompilerParams(vmem_limit_bytes=VLIM),
        cost_estimate=pl.CostEstimate(flops=10 * rows * rows * HEAD_DIM, bytes_accessed=20 * rows * HEAD_DIM,
                                      transcendentals=rows * rows // 2),
    )(k, v, k_t, q, q_t, d_o, d_ot, lse, dsum, cos_t, sin_t)


def dw_kernel(h_ref, g_ref, out_ref, acc_ref):
    step = pl.program_id(0)
    feat = h_ref.shape[1]
    tile = math.gcd(feat, 512)

    @pl.when(step == 0)
    def _():
        acc_ref[...] = jnp.zeros_like(acc_ref)

    def body(i, carry):
        cols = pl.ds(pl.multiple_of(i * tile, tile), tile)
        acc_ref[:, cols] += lax.dot_general(g_ref[...], h_ref[:, cols], (((0,), (0,)), ((), ())), preferred_element_type=F32)
        return carry

    lax.fori_loop(0, feat // tile, body, 0)

    @pl.when(step == pl.num_programs(0) - 1)
    def _():
        def flip(i, carry):
            rows = pl.ds(pl.multiple_of(i * tile, tile), tile)
            out_ref[rows, :] = acc_ref[:, rows].astype(BF16).T
            return carry

        lax.fori_loop(0, feat // tile, flip, 0)


def weight_grad(h_all, g_tok):
    rows, feat = h_all.shape
    width = g_tok.shape[1]
    bm = math.gcd(rows, 1024)
    return pl.pallas_call(
        dw_kernel, grid=(rows // bm,), name='weight_grad',
        in_specs=[pl.BlockSpec((bm, feat), lambda i: (i, 0)), pl.BlockSpec((bm, width), lambda i: (i, 0))],
        out_specs=pl.BlockSpec((feat, width), lambda i: (0, 0)), out_shape=jax.ShapeDtypeStruct((feat, width), BF16),
        scratch_shapes=[pltpu.VMEM((width, feat), F32)],
        compiler_params=pltpu.CompilerParams(vmem_limit_bytes=VLIM),
        cost_estimate=pl.CostEstimate(flops=2 * rows * feat * width, bytes_accessed=2 * rows * feat, transcendentals=0),
    )(h_all, g_tok)


def out_kernel(o_ref, w_ref, out_ref, acc_ref):
    step = pl.program_id(0)
    tile = math.gcd(w_ref.shape[1], 512)

    @pl.when(step == 0)
    def _():
        acc_ref[...] = jnp.zeros_like(acc_ref)

    def body(i, carry):
        cols = pl.ds(pl.multiple_of(i * tile, tile), tile)
        acc_ref[:, cols] += dot_f32(o_ref[0], w_ref[:, cols])
        return carry

    lax.fori_loop(0, w_ref.shape[1] // tile, body, 0)

    @pl.when(step == pl.num_programs(0) - 1)
    def _():
        out_ref[...] = acc_ref[...].astype(BF16)


def out_proj(o_own, w_o):
    devs, rows, width = o_own.shape
    feat = w_o.shape[1]
    return pl.pallas_call(
        out_kernel, grid=(devs,), name='out_proj',
        in_specs=[pl.BlockSpec((1, rows, width), lambda j: (j, 0, 0)), pl.BlockSpec((width, feat), lambda j: (j, 0))],
        out_specs=pl.BlockSpec((rows, feat), lambda j: (0, 0)), out_shape=jax.ShapeDtypeStruct((rows, feat), BF16),
        scratch_shapes=[pltpu.VMEM((rows, feat), F32)],
        compiler_params=pltpu.CompilerParams(vmem_limit_bytes=VLIM),
        cost_estimate=pl.CostEstimate(flops=2 * devs * rows * feat * width, bytes_accessed=2 * devs * feat * width, transcendentals=0),
    )(o_own, w_o)


def dh_kernel(heads, *refs):
    g_refs, w_refs = refs[:heads], refs[heads:heads + 3]
    x_ref, lnw_ref, dx_ref, dlnw_ref, acc_ref = refs[heads + 3:]
    step = pl.program_id(0)
    rows, feat = acc_ref.shape
    tile = math.gcd(feat, 512)

    @pl.when(step == 0)
    def _():
        acc_ref[...] = jnp.zeros_like(acc_ref)
        dlnw_ref[...] = jnp.zeros_like(dlnw_ref)

    def body(i, carry):
        cols = pl.ds(pl.multiple_of(i * tile, tile), tile)
        total = acc_ref[:, cols]
        for idx in range(3):
            lanes = slice(idx * HEAD_DIM, (idx + 1) * HEAD_DIM)
            lhs = jnp.concatenate([g_ref[0, :, lanes] for g_ref in g_refs], axis=1)
            total += lax.dot_general(lhs, w_refs[idx][cols, :], (((1,), (1,)), ((), ())), preferred_element_type=F32)
        acc_ref[:, cols] = total
        return carry

    lax.fori_loop(0, feat // tile, body, 0)

    @pl.when(step == pl.num_programs(0) - 1)
    def _():
        bm = math.gcd(rows, 64)
        weight = lnw_ref[...].astype(F32)

        def norm_bwd(i, carry):
            own = pl.ds(pl.multiple_of(i * bm, bm), bm)
            hid = x_ref[own, :].astype(F32)
            d_h = acc_ref[own, :]
            centered = hid - jnp.mean(hid, axis=-1, keepdims=True)
            rstd = lax.rsqrt(jnp.mean(centered * centered, axis=-1, keepdims=True) + LN_EPS)
            x_hat = centered * rstd
            dlnw_ref[...] += jnp.sum(d_h * x_hat, axis=0, keepdims=True)
            d_hat = d_h * weight
            mean_d = jnp.mean(d_hat, axis=-1, keepdims=True)
            mean_dx = jnp.mean(d_hat * x_hat, axis=-1, keepdims=True)
            dx_ref[own, :] = (rstd * (d_hat - mean_d - x_hat * mean_dx)).astype(BF16)
            return carry

        lax.fori_loop(0, rows // bm, norm_bwd, 0)


def hidden_grad(g_owns, weights, hidden, ln_weight):
    devs, rows, width = g_owns[0].shape
    heads = len(g_owns)
    feat = hidden.shape[1]
    whole = pl.BlockSpec((rows, feat), lambda j: (0, 0))
    vec = pl.BlockSpec((1, feat), lambda j: (0, 0))
    return pl.pallas_call(
        functools.partial(dh_kernel, heads), grid=(devs,), name='hidden_grad',
        in_specs=[pl.BlockSpec((1, rows, width), lambda j: (j, 0, 0))] * heads
        + [pl.BlockSpec((feat, heads * HEAD_DIM), lambda j: (0, j))] * 3 + [whole, vec],
        out_specs=[whole, vec],
        out_shape=[jax.ShapeDtypeStruct((rows, feat), BF16), jax.ShapeDtypeStruct((1, feat), F32)],
        scratch_shapes=[pltpu.VMEM((rows, feat), F32)],
        compiler_params=pltpu.CompilerParams(vmem_limit_bytes=VLIM),
        cost_estimate=pl.CostEstimate(flops=2 * devs * heads * rows * feat * width, bytes_accessed=6 * feat * feat,
                                      transcendentals=rows),
    )(*g_owns, *weights, hidden, ln_weight[None, :])


def copy_kernel(a_ref, out_ref):
    out_ref[...] = a_ref[...]


def copy_rows(val):
    rows, feat = val.shape
    spec = pl.BlockSpec((math.gcd(rows, 256), feat), lambda i: (i, 0))
    return pl.pallas_call(
        copy_kernel, grid=(rows // spec.block_shape[0],), name='copy_rows', in_specs=[spec], out_specs=spec,
        out_shape=jax.ShapeDtypeStruct(val.shape, val.dtype),
        cost_estimate=pl.CostEstimate(flops=rows * feat, bytes_accessed=4 * rows * feat, transcendentals=0),
    )(val)


def place_kernel(a_ref, *refs):
    for idx, out in enumerate(refs[-3:]):
        out[...] = a_ref[0, :, idx * HEAD_DIM:(idx + 1) * HEAD_DIM]


def place_slot(n, heads, gathered, grads):
    devs, feat, width = gathered.shape
    spec = pl.BlockSpec((feat, HEAD_DIM), lambda j: (0, j * heads + n))
    shape = jax.ShapeDtypeStruct((feat, devs * heads * HEAD_DIM), BF16)
    return pl.pallas_call(
        place_kernel, grid=(devs,), name='place',
        in_specs=[pl.BlockSpec((1, feat, width), lambda j: (j, 0, 0))] + [pl.BlockSpec(memory_space=pl.ANY)] * len(grads),
        out_specs=[spec] * 3, out_shape=[shape] * 3,
        input_output_aliases={1 + i: i for i in range(len(grads))},
        compiler_params=pltpu.CompilerParams(vmem_limit_bytes=VLIM),
        cost_estimate=pl.CostEstimate(flops=devs * feat * width, bytes_accessed=4 * devs * feat * width, transcendentals=0),
    )(gathered, *grads)


def solution(mesh):
    sp_size = mesh.shape['sp']
    row_spec = P(('dp', 'sp'), None)
    pos_spec = P(('dp', 'sp'))
    full_spec = P(None, None)
    grad_spec = P('dp', None)

    def layer_step(hidden, positions, d_attn, ln_weight, w_q, w_k, w_v, w_o):
        _, all_width = w_q.shape
        width = all_width // sp_size
        heads = width // HEAD_DIM
        me = lax.axis_index('sp')
        normed = layer_norm(hidden, ln_weight)
        h_all, pos_all = gather_tokens(normed, positions)
        cos_t, sin_t = rope_tables(pos_all)
        wo_cols = lax.dynamic_slice_in_dim(w_o, me * width, width, 0).T
        g_dep, h_all = lax.optimization_barrier((d_attn, h_all))
        g_all = lax.all_gather(g_dep, 'sp', axis=0, tiled=True)
        q, k, v, q_t, k_t, v_t = project(me, h_all, (w_q, w_k, w_v), cos_t, sin_t, heads)
        o_tok, o_t, lse = attn_fwd(k, q_t, v_t)

        row_major = Layout(major_to_minor=(0, 1, 2))

        def to_owner(val):
            val = with_layout_constraint(val.reshape(sp_size, -1, val.shape[1]), row_major)
            val = with_layout_constraint(lax.all_to_all(val, 'sp', 0, 0, tiled=True), row_major)
            return val

        o_tok, g_all = lax.optimization_barrier((o_tok, g_all))
        o_own = to_owner(o_tok)
        d_o, d_ot, dsum, dw_o = project_do(g_all, wo_cols, o_t, heads)
        dw_o = lax.all_gather(dw_o, 'sp', axis=0, tiled=True)
        dw_o = copy_rows(dw_o)
        attn_out = out_proj(o_own, w_o)
        d_ws = []
        g_owns = []
        for n in range(heads):
            g_tok = attn_bwd(n, k, v, k_t, q, q_t, d_o, d_ot, lse, dsum, cos_t, sin_t)
            d_w = weight_grad(h_all, g_tok)
            if n == heads - 1:
                g_tok, d_w = lax.optimization_barrier((g_tok, d_w))
            g_owns.append(to_owner(g_tok))
            d_ws.append(lax.all_gather(d_w, 'sp', axis=0))
        grads = place_slot(0, heads, d_ws[0], ())
        d_hid, d_lnw = hidden_grad(g_owns, (w_q, w_k, w_v), hidden, ln_weight)
        d_hid, d_ws[1:] = lax.optimization_barrier((d_hid, d_ws[1:]))
        for n in range(1, heads):
            grads = place_slot(n, heads, d_ws[n], grads)
        d_lnw = lax.psum(d_lnw[0], 'sp')
        return (attn_out, d_hid, d_lnw.astype(BF16), grads[0], grads[1], grads[2], dw_o)

    return jax.shard_map(layer_step, mesh=mesh,
                         in_specs=(row_spec, pos_spec, row_spec, P(None), full_spec, full_spec, full_spec, full_spec),
                         out_specs=(row_spec, row_spec, P('dp'), grad_spec, grad_spec, grad_spec, grad_spec),
                         check_vma=False)
```
